8 devices in a mesh: dp: 2 (over z, y), cp: 4 (over x, core).
Axes of the slice: x: 2, y: 2, z: 1, core: 2. Of those that a mesh axis runs over, the one named last changes fastest.
Arguments:
- x_in: bfloat16 [2048, 1536], P(('dp', 'cp')), parts along dimension 0
- dy_in: bfloat16 [2048, 1536], P(('dp', 'cp')), parts along dimension 0
- w_q: bfloat16 [1536, 1536], replicated
- w_k: bfloat16 [1536, 256], replicated
- w_v: bfloat16 [1536, 256], replicated
- w_o: bfloat16 [1536, 1536], replicated
Outputs:
- output 1: bfloat16 [2048, 1536], P(('dp', 'cp')), parts along dimension 0
- output 2: bfloat16 [2048, 1536], P(('dp', 'cp')), parts along dimension 0
There are 2 independent parts. The reference program is written for one: setup_inputs(seed, part) draws one part's arguments, and reference() takes and returns one part's arrays. A program takes and returns all parts, laid end to end along the dimension named above; an argument that names none is the same for every part.
All inputs are finite; a program needn't handle non-finite values.
Results may differ from the reference program's by a relative error of at most 0.0108757.
Values are sent between devices in bfloat16 or wider.
A program may use at most 1 GiB of HBM per device.

```python
import math
import jax
import jax.numpy as jnp
from jax import lax

SEQ_LEN = 1024
D_MODEL = 1536
Q_HEADS = 12
KV_HEADS = 2
HEAD_DIM = 128
QUERY_BLOCK = 128

Q_GROUP = Q_HEADS // KV_HEADS
SCORE_GAIN = (0.75 * math.log(SEQ_LEN)) ** 0.25


def setup_inputs(seed: int = 0, part: int = 0) -> dict:
    key_base = jax.random.key(seed)
    key_part = jax.random.fold_in(key_base, part)
    key_x, key_dy = jax.random.split(key_part)
    key_wq, key_wk, key_wv, key_wo = jax.random.split(jax.random.key(seed + 1), 4)
    in_scale = D_MODEL ** -0.5
    out_scale = (Q_HEADS * HEAD_DIM) ** -0.5
    x_in = jax.random.normal(key_x, (SEQ_LEN, D_MODEL), jnp.float32).astype(jnp.bfloat16)
    dy_in = jax.random.normal(key_dy, (SEQ_LEN, D_MODEL), jnp.float32).astype(jnp.bfloat16)
    w_q = (jax.random.normal(key_wq, (D_MODEL, Q_HEADS * HEAD_DIM), jnp.float32) * (in_scale * SCORE_GAIN)).astype(jnp.bfloat16)
    w_k = (jax.random.normal(key_wk, (D_MODEL, KV_HEADS * HEAD_DIM), jnp.float32) * (in_scale * SCORE_GAIN)).astype(jnp.bfloat16)
    w_v = (jax.random.normal(key_wv, (D_MODEL, KV_HEADS * HEAD_DIM), jnp.float32) * in_scale).astype(jnp.bfloat16)
    w_o = (jax.random.normal(key_wo, (Q_HEADS * HEAD_DIM, D_MODEL), jnp.float32) * out_scale).astype(jnp.bfloat16)
    return {"x_in": x_in, "dy_in": dy_in, "w_q": w_q, "w_k": w_k, "w_v": w_v, "w_o": w_o}


def project(rows_in, weight):
    return jnp.dot(rows_in, weight, preferred_element_type=jnp.float32).astype(jnp.bfloat16)


def reference(x_in, dy_in, w_q, w_k, w_v, w_o):
    score_scale = HEAD_DIM ** -0.5
    n_blocks = SEQ_LEN // QUERY_BLOCK
    q_rows = project(x_in, w_q).reshape(n_blocks, QUERY_BLOCK, KV_HEADS, Q_GROUP, HEAD_DIM)
    k_rows = project(x_in, w_k).reshape(SEQ_LEN, KV_HEADS, HEAD_DIM).astype(jnp.float32)
    v_rows = project(x_in, w_v).reshape(SEQ_LEN, KV_HEADS, HEAD_DIM).astype(jnp.float32)

    def forward_block(q_blk):
        q_f = q_blk.astype(jnp.float32)
        scores = jnp.einsum("thjd,uhd->thju", q_f, k_rows) * score_scale
        lse_blk = jax.nn.logsumexp(scores, axis=-1, keepdims=True)
        prob_bf = jnp.exp(scores - lse_blk).astype(jnp.bfloat16)
        out_blk = jnp.einsum("thju,uhd->thjd", prob_bf.astype(jnp.float32), v_rows).astype(jnp.bfloat16)
        return out_blk, lse_blk

    out_blocks, lse_blocks = lax.map(forward_block, q_rows)
    out_flat = out_blocks.reshape(SEQ_LEN, Q_HEADS * HEAD_DIM)
    y_out = project(out_flat, w_o)
    do_flat = jnp.dot(dy_in, w_o.T, preferred_element_type=jnp.float32).astype(jnp.bfloat16)
    do_blocks = do_flat.reshape(n_blocks, QUERY_BLOCK, KV_HEADS, Q_GROUP, HEAD_DIM)

    def backward_block(acc_pair, block_in):
        dk_acc, dv_acc = acc_pair
        q_blk, out_blk, do_blk, lse_blk = block_in
        q_f = q_blk.astype(jnp.float32)
        do_f = do_blk.astype(jnp.float32)
        scores = jnp.einsum("thjd,uhd->thju", q_f, k_rows) * score_scale
        prob_f = jnp.exp(scores - lse_blk).astype(jnp.bfloat16).astype(jnp.float32)
        row_delta = jnp.sum(do_f * out_blk.astype(jnp.float32), axis=-1, keepdims=True)
        dprob = jnp.einsum("thjd,uhd->thju", do_f, v_rows)
        dscore = (prob_f * (dprob - row_delta)).astype(jnp.bfloat16).astype(jnp.float32)
        dq_blk = (jnp.einsum("thju,uhd->thjd", dscore, k_rows) * score_scale).astype(jnp.bfloat16)
        dk_acc = dk_acc + jnp.einsum("thju,thjd->uhd", dscore, q_f) * score_scale
        dv_acc = dv_acc + jnp.einsum("thju,thjd->uhd", prob_f, do_f)
        return (dk_acc, dv_acc), dq_blk

    zero_acc = jnp.zeros((SEQ_LEN, KV_HEADS, HEAD_DIM), jnp.float32)
    acc_final, dq_blocks = lax.scan(backward_block, (zero_acc, zero_acc), (q_rows, out_blocks, do_blocks, lse_blocks))
    dq_flat = dq_blocks.reshape(SEQ_LEN, Q_HEADS * HEAD_DIM)
    dk_flat = acc_final[0].astype(jnp.bfloat16).reshape(SEQ_LEN, KV_HEADS * HEAD_DIM)
    dv_flat = acc_final[1].astype(jnp.bfloat16).reshape(SEQ_LEN, KV_HEADS * HEAD_DIM)
    dx_acc = (jnp.dot(dq_flat, w_q.T, preferred_element_type=jnp.float32)
              + jnp.dot(dk_flat, w_k.T, preferred_element_type=jnp.float32)
              + jnp.dot(dv_flat, w_v.T, preferred_element_type=jnp.float32))
    return y_out, dx_acc.astype(jnp.bfloat16)
```

```python
import functools
import math

import jax
import jax.numpy as jnp
from jax import lax
from jax.experimental import pallas as pl
from jax.experimental.pallas import tpu as pltpu
from jax.sharding import PartitionSpec as P

HEAD_DIM = 128
MESH = pl.DeviceIdType.MESH
F32 = jnp.float32
BF16 = jnp.bfloat16
NT = (((1,), (1,)), ((), ()))
NN = (((1,), (0,)), ((), ()))


def mm(a, b, dims=NN):
    return lax.dot_general(a, b, dims, preferred_element_type=F32)


def kernel(rows, d_model, q_heads, kv_heads,
           x_hbm, dy_hbm, wq_hbm, wk_hbm, wv_hbm, wo_hbm,
           y_hbm, dx_hbm,
           x_v, dy_v, wq_v, wk_v, wv_v, wo_v,
           qs, dot_v, k_all, v_all, kt, vt, pt, ds_t, s_buf, o_v, ot_v, dq_v,
           part, recv_a, recv_b, recv_c, send_c, dx_acc, y_v, dx_v,
           in_sem, out_sem, ag_send, ag_recv, rs_send, rs_recv):
    group = q_heads // kv_heads
    d = HEAD_DIM
    n_keys = 4 * rows
    half = group * rows
    scale = d ** -0.5
    gain = scale * math.log2(math.e)

    me = lax.axis_index("cp")
    core = lax.rem(me, 2)
    partner = me + 1 - 2 * core
    cross = lax.rem(me + 2, 4)

    barrier = pltpu.get_barrier_semaphore()
    for peer in (partner, cross):
        pl.semaphore_signal(barrier, inc=1, device_id={"cp": peer}, device_id_type=MESH)

    qcols = q_heads * d // 2
    loads = [
        pltpu.make_async_copy(x_hbm, x_v, in_sem.at[0]),
        pltpu.make_async_copy(wk_hbm, wk_v, in_sem.at[1]),
        pltpu.make_async_copy(wv_hbm, wv_v, in_sem.at[2]),
        pltpu.make_async_copy(wq_hbm.at[:, :qcols], wq_v.at[:, :qcols], in_sem.at[3]),
        pltpu.make_async_copy(wq_hbm.at[:, qcols:], wq_v.at[:, qcols:], in_sem.at[4]),
        pltpu.make_async_copy(dy_hbm, dy_v, in_sem.at[5]),
        pltpu.make_async_copy(wo_hbm.at[:qcols], wo_v.at[:qcols], in_sem.at[6]),
        pltpu.make_async_copy(wo_hbm.at[qcols:], wo_v.at[qcols:], in_sem.at[7]),
    ]
    for copy in loads:
        copy.start()

    def item(i):
        return (k_all if i % 2 == 0 else v_all).at[i // 2]

    def slot(i, s):
        return item(i).at[pl.ds(s * rows, rows)]

    def ag_copy(i, hop):
        src, dst, peer = ((0, 1, partner), (0, 2, cross), (2, 3, partner))[hop]
        return pltpu.make_async_remote_copy(
            src_ref=slot(i, src), dst_ref=slot(i, dst),
            send_sem=ag_send.at[i, hop], recv_sem=ag_recv.at[i, hop],
            device_id={"cp": peer}, device_id_type=MESH)

    def forward(i):
        ag_copy(i, 1).wait_recv()
        ag_copy(i, 2).start()

    def finish_item(i):
        ag_copy(i, 0).wait_recv()
        ag_copy(i, 2).wait_recv()
        (kt if i % 2 == 0 else vt)[i // 2] = item(i)[...].T

    loads[0].wait()
    for w, copy, kv_ref in ((wk_v, loads[1], k_all), (wv_v, loads[2], v_all)):
        copy.wait()
        out = mm(x_v[...], w[...]).astype(BF16)
        for h in range(kv_heads):
            kv_ref[h, :rows, :] = out[:, h * d:(h + 1) * d]
    pl.semaphore_wait(barrier, 2)
    for i in range(2 * kv_heads):
        ag_copy(i, 1).start()
        ag_copy(i, 0).start()

    for n in range(q_heads // 2):
        if n == 0:
            loads[3].wait()
        if n == q_heads // 4:
            loads[4].wait()
        out = mm(x_v[...], wq_v[:, n * 2 * d:(n + 1) * 2 * d]).astype(BF16)
        for t in range(2):
            head = 2 * n + t
            h, j = head // group, head % group
            qs[h, j * rows:(j + 1) * rows, :] = out[:, t * d:(t + 1) * d]

    loads[5].wait()
    for n in range(q_heads // 2):
        if n == 0:
            loads[6].wait()
        if n == q_heads // 4:
            forward(0)
            loads[7].wait()
        out = mm(wo_v[n * 2 * d:(n + 1) * 2 * d, :], dy_v[...], NT).astype(BF16)
        for t in range(2):
            head = 2 * n + t
            h, j = head // group, head % group
            dot_v[h, :, j * rows:(j + 1) * rows] = out[t * d:(t + 1) * d, :]

    def probs(h, j):
        cols = pl.ds(pl.multiple_of(j * rows, rows), rows)
        q = qs[h, cols, :]
        m8 = None
        for c in range(4):
            s = mm(k_all[h, c * rows:(c + 1) * rows, :], q, NT)
            s_buf[c * rows:(c + 1) * rows, :] = s
            t8 = jnp.max(s.reshape(rows // 8, 8, rows), axis=0)
            m8 = t8 if m8 is None else jnp.maximum(m8, t8)
        mk = jnp.max(m8, axis=0, keepdims=True) * gain
        l8 = jnp.zeros((8, rows), F32)
        for c in range(4):
            e = jnp.exp2(s_buf[c * rows:(c + 1) * rows, :] * gain - mk)
            s_buf[c * rows:(c + 1) * rows, :] = e
            l8 = l8 + jnp.sum(e.reshape(rows // 8, 8, rows), axis=0)
        inv = 1.0 / jnp.sum(l8, axis=0, keepdims=True)
        for c in range(4):
            pt[h, c * rows:(c + 1) * rows, cols] = (s_buf[c * rows:(c + 1) * rows, :] * inv).astype(BF16)

    def outs(h, j):
        cols = pl.ds(pl.multiple_of(j * rows, rows), rows)
        head = pl.ds(pl.multiple_of((h * group + j) * d, d), d)
        o_t = mm(vt[h], pt[h, :, cols]).astype(BF16)
        o_v[:, head] = o_t.T
        do_t = dot_v[h, :, cols]
        delta = jnp.sum(do_t.astype(F32) * o_t.astype(F32), axis=0, keepdims=True)
        for c in range(4):
            dp = mm(v_all[h, c * rows:(c + 1) * rows, :], do_t)
            p = pt[h, c * rows:(c + 1) * rows, cols].astype(F32)
            ds_t[h, c * rows:(c + 1) * rows, cols] = (p * (dp - delta)).astype(BF16)

    def dqs(h, j):
        cols = pl.ds(pl.multiple_of(j * rows, rows), rows)
        head = pl.ds(pl.multiple_of((h * group + j) * d, d), d)
        dq_t = (mm(kt[h], ds_t[h, :, cols]) * scale).astype(BF16)
        dq_v[:, head] = dq_t.T

    def grads(r, s):
        h = r % kv_heads
        block = slice(s * rows, (s + 1) * rows)
        if r < kv_heads:
            return mm(pt[h, block, :], dot_v[h], NT)
        return mm(ds_t[h, block, :], qs[h])

    def rs_copy(r, kind):
        src, dst_ref, peer = ((part.at[r, 3], recv_a.at[r], partner),
                              (part.at[r, 1], recv_b.at[r], partner),
                              (send_c.at[r], recv_c.at[r], cross))[kind]
        return pltpu.make_async_remote_copy(
            src_ref=src, dst_ref=dst_ref,
            send_sem=rs_send.at[r, kind], recv_sem=rs_recv.at[r, kind],
            device_id={"cp": peer}, device_id_type=MESH)

    def reduce_first(r):
        part[r, 3] = grads(r, 3)
        rs_copy(r, 0).start()
        part[r, 2] = grads(r, 2)

    def reduce_cross(r):
        rs_copy(r, 0).wait_recv()
        send_c[r] = part[r, 2] + recv_a[r]
        rs_copy(r, 2).start()

    def reduce_local(r):
        part[r, 1] = grads(r, 1)
        rs_copy(r, 1).start()
        part[r, 0] = grads(r, 0)

    def loop(body, h, lo, hi):
        def step(j, carry):
            body(h, j)
            return carry
        lax.fori_loop(lo, hi, step, 0)

    finish_item(0)
    loop(probs, 0, 0, 3)
    forward(1)
    loop(probs, 0, 3, 6)
    forward(2)
    reduce_first(0)
    finish_item(1)
    finish_item(2)
    loop(probs, 1, 0, 3)
    reduce_cross(0)
    forward(3)
    loop(probs, 1, 3, 6)
    reduce_first(1)
    finish_item(3)
    loop(outs, 0, 0, 3)
    reduce_cross(1)
    loop(outs, 0, 3, 6)
    reduce_first(2)
    loop(outs, 1, 0, 3)
    reduce_cross(2)
    loop(outs, 1, 3, 6)
    reduce_first(3)
    reduce_local(0)
    reduce_cross(3)
    for r in range(1, 2 * kv_heads):
        reduce_local(r)
    for h in range(kv_heads):
        loop(dqs, h, 0, group)

    y_copies = []
    for n in range(d_model // 256):
        cols = slice(n * 256, (n + 1) * 256)
        y_v[:, cols] = mm(o_v[...], wo_v[:, cols]).astype(BF16)
        copy = pltpu.make_async_copy(y_v.at[:, cols], y_hbm.at[:, cols], out_sem.at[n])
        copy.start()
        y_copies.append(copy)
    for n in range(d_model // 256):
        cols = slice(n * 256, (n + 1) * 256)
        dx_acc[:, cols] = mm(dq_v[...], wq_v[cols, :], NT)

    own = []
    for r in range(2 * kv_heads):
        rs_copy(r, 1).wait_recv()
        rs_copy(r, 2).wait_recv()
        total = part[r, 0] + recv_b[r] + recv_c[r]
        if r >= kv_heads:
            total = total * scale
        own.append(total.astype(BF16))
    dv = jnp.concatenate(own[:kv_heads], axis=1)
    dk = jnp.concatenate(own[kv_heads:], axis=1)
    dx_copies = []
    for n in range(d_model // 256):
        cols = slice(n * 256, (n + 1) * 256)
        total = dx_acc[:, cols] + mm(dk, wk_v[cols, :], NT) + mm(dv, wv_v[cols, :], NT)
        dx_v[:, cols] = total.astype(BF16)
        copy = pltpu.make_async_copy(dx_v.at[:, cols], dx_hbm.at[:, cols], out_sem.at[6 + n])
        copy.start()
        dx_copies.append(copy)

    for i in range(2 * kv_heads):
        for hop in range(3):
            ag_copy(i, hop).wait_send()
    for r in range(2 * kv_heads):
        for kind in range(3):
            rs_copy(r, kind).wait_send()
    for copy in y_copies + dx_copies:
        copy.wait()


def solution(mesh):
    row_spec = P(("dp", "cp"), None)
    full_spec = P(None, None)

    def local_body(x_loc, dy_loc, w_q, w_k, w_v, w_o):
        rows, d_model = x_loc.shape
        d = HEAD_DIM
        q_heads = w_q.shape[1] // d
        kv_heads = w_k.shape[1] // d
        group = q_heads // kv_heads
        n_keys = 4 * rows
        qw = q_heads * d
        any_spec = pl.BlockSpec(memory_space=pl.ANY)
        out = jax.ShapeDtypeStruct((rows, d_model), BF16)
        items = 2 * kv_heads
        return pl.pallas_call(
            functools.partial(kernel, rows, d_model, q_heads, kv_heads),
            out_shape=(out, out),
            in_specs=[any_spec] * 6,
            out_specs=(any_spec, any_spec),
            scratch_shapes=[
                pltpu.VMEM((rows, d_model), BF16),
                pltpu.VMEM((rows, d_model), BF16),
                pltpu.VMEM((d_model, qw), BF16),
                pltpu.VMEM((d_model, kv_heads * d), BF16),
                pltpu.VMEM((d_model, kv_heads * d), BF16),
                pltpu.VMEM((qw, d_model), BF16),
                pltpu.VMEM((kv_heads, group * rows, d), BF16),
                pltpu.VMEM((kv_heads, d, group * rows), BF16),
                pltpu.VMEM((kv_heads, n_keys, d), BF16),
                pltpu.VMEM((kv_heads, n_keys, d), BF16),
                pltpu.VMEM((kv_heads, d, n_keys), BF16),
                pltpu.VMEM((kv_heads, d, n_keys), BF16),
                pltpu.VMEM((kv_heads, n_keys, group * rows), BF16),
                pltpu.VMEM((kv_heads, n_keys, group * rows), BF16),
                pltpu.VMEM((n_keys, rows), F32),
                pltpu.VMEM((rows, qw), BF16),
                pltpu.VMEM((q_heads, d, rows), BF16),
                pltpu.VMEM((rows, qw), BF16),
                pltpu.VMEM((items, 4, rows, d), F32),
                pltpu.VMEM((items, rows, d), F32),
                pltpu.VMEM((items, rows, d), F32),
                pltpu.VMEM((items, rows, d), F32),
                pltpu.VMEM((items, rows, d), F32),
                pltpu.VMEM((rows, d_model), F32),
                pltpu.VMEM((rows, d_model), BF16),
                pltpu.VMEM((rows, d_model), BF16),
                pltpu.SemaphoreType.DMA((8,)),
                pltpu.SemaphoreType.DMA((12,)),
                pltpu.SemaphoreType.DMA((items, 3)),
                pltpu.SemaphoreType.DMA((items, 3)),
                pltpu.SemaphoreType.DMA((items, 3)),
                pltpu.SemaphoreType.DMA((items, 3)),
            ],
            compiler_params=pltpu.CompilerParams(
                collective_id=0, has_side_effects=True,
                vmem_limit_bytes=60 * 1024 * 1024),
        )(x_loc, dy_loc, w_q, w_k, w_v, w_o)

    return jax.shard_map(local_body, mesh=mesh,
                         in_specs=(row_spec, row_spec, full_spec, full_spec, full_spec, full_spec),
                         out_specs=(row_spec, row_spec), check_vma=False)
```

```python
import functools
import math

import jax
import jax.numpy as jnp
from jax import lax
from jax.experimental import pallas as pl
from jax.experimental.pallas import tpu as pltpu
from jax.sharding import PartitionSpec as P

HEAD_DIM = 128
CHUNK = 128
MESH = pl.DeviceIdType.MESH
F32 = jnp.float32
BF16 = jnp.bfloat16
NT = (((1,), (1,)), ((), ()))
NN = (((1,), (0,)), ((), ()))


def mm(a, b, dims=NN):
    return lax.dot_general(a, b, dims, preferred_element_type=F32)


def kernel(rows, d_model, q_heads, kv_heads,
           x_hbm, dy_hbm, wq_hbm, wk_hbm, wv_hbm, wo_hbm,
           y_v, dx_v,
           x_v, dy_v, wq_v, wk_v, wv_v, wo_v,
           qs, dot_v, k_all, v_all, kt, vt, pt, ds_t, e_buf, m_buf, l_buf, o_v, dq_v,
           part, recv_a, recv_b, recv_c, send_c, dx_acc,
           in_sem, ag_send, ag_recv, rs_send, rs_recv):
    group = q_heads // kv_heads
    d = HEAD_DIM
    n_keys = 4 * rows
    half = group * rows
    scale = d ** -0.5
    gain = scale * math.log2(math.e)

    me = lax.axis_index("cp")
    core = lax.rem(me, 2)
    partner = me + 1 - 2 * core
    cross = lax.rem(me + 2, 4)

    barrier = pltpu.get_barrier_semaphore()
    for peer in (partner, cross):
        pl.semaphore_signal(barrier, inc=1, device_id={"cp": peer}, device_id_type=MESH)

    qcols = q_heads * d // 2
    loads = [
        pltpu.make_async_copy(wk_hbm, wk_v, in_sem.at[1]),
        pltpu.make_async_copy(x_hbm, x_v, in_sem.at[0]),
        pltpu.make_async_copy(wv_hbm, wv_v, in_sem.at[2]),
        pltpu.make_async_copy(wq_hbm.at[:, :qcols], wq_v.at[:, :qcols], in_sem.at[3]),
        pltpu.make_async_copy(wq_hbm.at[:, qcols:], wq_v.at[:, qcols:], in_sem.at[4]),
        pltpu.make_async_copy(dy_hbm, dy_v, in_sem.at[5]),
        pltpu.make_async_copy(wo_hbm.at[:qcols], wo_v.at[:qcols], in_sem.at[6]),
        pltpu.make_async_copy(wo_hbm.at[qcols:], wo_v.at[qcols:], in_sem.at[7]),
    ]
    for copy in loads:
        copy.start()

    def item(i):
        return (k_all if i % 2 == 0 else v_all).at[i // 2]

    def slot(i, s):
        return item(i).at[pl.ds(s * rows, rows)]

    def ag_copy(i, hop):
        src, dst, peer = ((0, 1, partner), (0, 2, cross), (2, 3, partner))[hop]
        return pltpu.make_async_remote_copy(
            src_ref=slot(i, src), dst_ref=slot(i, dst),
            send_sem=ag_send.at[i, hop], recv_sem=ag_recv.at[i, hop],
            device_id={"cp": peer}, device_id_type=MESH)

    def forward(i):
        ag_copy(i, 1).wait_recv()
        ag_copy(i, 2).start()

    def transpose_item(i, ref):
        for s in range(4):
            ref[i // 2, :, s * rows:(s + 1) * rows] = slot(i, s)[...].T

    def head_of(i):
        h, j = i // group, i % group
        return h, slice(j * rows, (j + 1) * rows), slice(i * d, (i + 1) * d)

    def project_q(n):
        out = mm(x_v[...], wq_v[:, n * 2 * d:(n + 1) * 2 * d]).astype(BF16)
        for t in range(2):
            h, cols, _ = head_of(2 * n + t)
            qs[h, cols, :] = out[:, t * d:(t + 1) * d]

    def project_do(n):
        out = mm(wo_v[n * 2 * d:(n + 1) * 2 * d, :], dy_v[...], NT).astype(BF16)
        for t in range(2):
            h, cols, _ = head_of(2 * n + t)
            dot_v[h, :, cols] = out[t * d:(t + 1) * d, :]

    per_slot = rows // CHUNK

    def scores(i, s):
        h, cols, _ = head_of(i)
        j = i % group
        raw = mm(k_all[h, s * rows:(s + 1) * rows, :], qs[h, cols, :], NT)
        for c in range(per_slot):
            t = raw[c * CHUNK:(c + 1) * CHUNK] * gain
            t = t.reshape(CHUNK // 8, 8, rows)
            m8 = jnp.max(t, axis=0)
            e = jnp.exp2(t - m8[None])
            e_buf[j, s * rows + c * CHUNK:s * rows + (c + 1) * CHUNK, :] = e.reshape(CHUNK, rows)
            m_buf[j, s * per_slot + c] = m8
            l_buf[j, s * per_slot + c] = jnp.sum(e, axis=0)

    def finalize(i):
        h, cols, _ = head_of(i)
        j = i % group
        n_chunks = 4 * per_slot
        top = jnp.max(jnp.max(m_buf[j], axis=0), axis=0, keepdims=True)
        factor = [jnp.exp2(m_buf[j, c] - top) for c in range(n_chunks)]
        total = factor[0] * l_buf[j, 0]
        for c in range(1, n_chunks):
            total = total + factor[c] * l_buf[j, c]
        inv = 1.0 / jnp.sum(total, axis=0, keepdims=True)
        for c in range(n_chunks):
            f8 = factor[c] * inv
            e = e_buf[j, c * CHUNK:(c + 1) * CHUNK, :].reshape(CHUNK // 8, 8, rows)
            pt[h, c * CHUNK:(c + 1) * CHUNK, cols] = (e * f8[None]).reshape(CHUNK, rows).astype(BF16)

    def outs(i):
        h, cols, feats = head_of(i)
        o_t = mm(vt[h], pt[h, :, cols]).astype(BF16)
        o_v[:, feats] = o_t.T
        do_t = dot_v[h, :, cols]
        delta = jnp.sum(do_t.astype(F32) * o_t.astype(F32), axis=0, keepdims=True)
        for s in range(4):
            keys = slice(s * rows, (s + 1) * rows)
            dp = mm(v_all[h, keys, :], do_t)
            ds_t[h, keys, cols] = (pt[h, keys, cols].astype(F32) * (dp - delta)).astype(BF16)

    def dqs(i):
        h, cols, feats = head_of(i)
        dq_v[:, feats] = (mm(kt[h], ds_t[h, :, cols]) * scale).astype(BF16).T

    def grads(r, lo, hi):
        h = r % kv_heads
        block = slice(lo * rows, hi * rows)
        if r < kv_heads:
            out = mm(pt[h, block, :], dot_v[h], NT)
        else:
            out = mm(ds_t[h, block, :], qs[h])
        for s in range(lo, hi):
            part[r, s] = out[(s - lo) * rows:(s - lo + 1) * rows]

    def rs_copy(r, kind):
        src, dst, peer = ((part.at[r, 3], recv_a.at[r], partner),
                          (part.at[r, 1], recv_b.at[r], partner),
                          (send_c.at[r], recv_c.at[r], cross))[kind]
        return pltpu.make_async_remote_copy(
            src_ref=src, dst_ref=dst,
            send_sem=rs_send.at[r, kind], recv_sem=rs_recv.at[r, kind],
            device_id={"cp": peer}, device_id_type=MESH)

    def reduce_cross(r):
        rs_copy(r, 0).wait_recv()
        send_c[r] = part[r, 2] + recv_a[r]
        rs_copy(r, 2).start()

    first = range(group)
    second = range(group, q_heads)

    loads[0].wait()
    loads[1].wait()
    for w, copy, kv_ref in ((wk_v, None, k_all), (wv_v, loads[2], v_all)):
        if copy is not None:
            copy.wait()
        out = mm(x_v[...], w[...]).astype(BF16)
        for h in range(kv_heads):
            kv_ref[h, :rows, :] = out[:, h * d:(h + 1) * d]
        if copy is None:
            pl.semaphore_wait(barrier, 2)
        for h in range(kv_heads):
            i = 2 * h + (0 if copy is None else 1)
            ag_copy(i, 1).start()
            ag_copy(i, 0).start()

    loads[3].wait()
    for n in range(q_heads // 4):
        project_q(n)
    loads[4].wait()
    ag_copy(0, 0).wait_recv()
    for n in range(q_heads // 4):
        project_q(q_heads // 4 + n)
        for s in (0, 1):
            scores(n, s)
    loads[5].wait()
    loads[6].wait()
    for n in range(q_heads // 4):
        project_do(n)
        for s in (0, 1):
            scores(q_heads // 4 + n, s)
    loads[7].wait()
    forward(0)
    for n in range(q_heads // 4):
        project_do(q_heads // 4 + n)
        scores(2 * n, 2)
        scores(2 * n + 1, 2)
    ag_copy(0, 2).wait_recv()
    for i in first:
        scores(i, 3)
    for i in first:
        finalize(i)
    forward(1)
    grads(0, 3, 4)
    rs_copy(0, 0).start()
    grads(0, 2, 3)
    ag_copy(2, 0).wait_recv()
    for n in range(group):
        scores(group + n, 0)
        scores(group + n, 1)
        if n == 0:
            grads(0, 1, 2)
        if n == 2:
            grads(0, 0, 1)
    forward(2)
    reduce_cross(0)
    rs_copy(0, 1).start()
    ag_copy(1, 0).wait_recv()
    ag_copy(1, 2).wait_recv()
    transpose_item(1, vt)
    for i in first:
        outs(i)
        scores(group + i, 2)
    forward(3)
    ag_copy(2, 2).wait_recv()
    grads(2, 3, 4)
    for i in second:
        scores(i, 3)
    rs_copy(2, 0).start()
    grads(2, 2, 3)
    for i in second:
        finalize(i)
    grads(1, 3, 4)
    rs_copy(1, 0).start()
    grads(1, 2, 3)
    ag_copy(3, 0).wait_recv()
    ag_copy(3, 2).wait_recv()
    reduce_cross(2)
    transpose_item(3, vt)
    for i in range(group, group + group // 2):
        outs(i)
    reduce_cross(1)
    for i in range(group + group // 2, q_heads):
        outs(i)
    grads(3, 3, 4)
    rs_copy(3, 0).start()
    grads(3, 2, 3)
    for r in (2, 1):
        grads(r, 0, 2)
        rs_copy(r, 1).start()
    reduce_cross(3)
    grads(3, 0, 2)
    rs_copy(3, 1).start()
    transpose_item(0, kt)
    transpose_item(2, kt)
    for i in range(q_heads):
        dqs(i)
    for n in range(d_model // 256):
        cols = slice(n * 256, (n + 1) * 256)
        y_v[:, cols] = mm(o_v[...], wo_v[:, cols]).astype(BF16)
    for n in range(d_model // 256):
        cols = slice(n * 256, (n + 1) * 256)
        dx_acc[:, cols] = mm(dq_v[...], wq_v[cols, :], NT)

    def own(r):
        rs_copy(r, 1).wait_recv()
        rs_copy(r, 2).wait_recv()
        total = part[r, 0] + recv_b[r] + recv_c[r]
        if r >= kv_heads:
            total = total * scale
        return total.astype(BF16)

    for r in (0, 2, 1):
        g = own(r)
        h = r % kv_heads
        w = wv_v if r < kv_heads else wk_v
        for n in range(d_model // 256):
            cols = slice(n * 256, (n + 1) * 256)
            dx_acc[:, cols] += mm(g, w[cols, h * d:(h + 1) * d], NT)
    g = own(3)
    for n in range(d_model // 256):
        cols = slice(n * 256, (n + 1) * 256)
        total = dx_acc[:, cols] + mm(g, wk_v[cols, d:2 * d], NT)
        dx_v[:, cols] = total.astype(BF16)

    for i in range(2 * kv_heads):
        for hop in range(3):
            ag_copy(i, hop).wait_send()
    for r in range(2 * kv_heads):
        for kind in range(3):
            rs_copy(r, kind).wait_send()


def write_out(y_v, dx_v, y_hbm, dx_hbm, sem):
    copies = [pltpu.make_async_copy(y_v, y_hbm, sem.at[0]),
              pltpu.make_async_copy(dx_v, dx_hbm, sem.at[1])]
    for copy in copies:
        copy.start()
    for copy in copies:
        copy.wait()


def solution(mesh):
    row_spec = P(("dp", "cp"), None)
    full_spec = P(None, None)

    def local_body(x_loc, dy_loc, w_q, w_k, w_v, w_o):
        rows, d_model = x_loc.shape
        d = HEAD_DIM
        q_heads = w_q.shape[1] // d
        kv_heads = w_k.shape[1] // d
        group = q_heads // kv_heads
        n_keys = 4 * rows
        qw = q_heads * d
        hbm = pl.BlockSpec(memory_space=pltpu.HBM)
        vmem = pl.BlockSpec(memory_space=pltpu.VMEM)
        out = jax.ShapeDtypeStruct((rows, d_model), BF16)
        items = 2 * kv_heads
        y_v, dx_v = pl.pallas_call(
            functools.partial(kernel, rows, d_model, q_heads, kv_heads),
            out_shape=(out, out),
            in_specs=[hbm] * 6,
            out_specs=(vmem, vmem),
            scratch_shapes=[
                pltpu.VMEM((rows, d_model), BF16),
                pltpu.VMEM((rows, d_model), BF16),
                pltpu.VMEM((d_model, qw), BF16),
                pltpu.VMEM((d_model, kv_heads * d), BF16),
                pltpu.VMEM((d_model, kv_heads * d), BF16),
                pltpu.VMEM((qw, d_model), BF16),
                pltpu.VMEM((kv_heads, group * rows, d), BF16),
                pltpu.VMEM((kv_heads, d, group * rows), BF16),
                pltpu.VMEM((kv_heads, n_keys, d), BF16),
                pltpu.VMEM((kv_heads, n_keys, d), BF16),
                pltpu.VMEM((kv_heads, d, n_keys), BF16),
                pltpu.VMEM((kv_heads, d, n_keys), BF16),
                pltpu.VMEM((kv_heads, n_keys, group * rows), BF16),
                pltpu.VMEM((kv_heads, n_keys, group * rows), BF16),
                pltpu.VMEM((group, n_keys, rows), F32),
                pltpu.VMEM((group, n_keys // CHUNK, 8, rows), F32),
                pltpu.VMEM((group, n_keys // CHUNK, 8, rows), F32),
                pltpu.VMEM((rows, qw), BF16),
                pltpu.VMEM((rows, qw), BF16),
                pltpu.VMEM((items, 4, rows, d), F32),
                pltpu.VMEM((items, rows, d), F32),
                pltpu.VMEM((items, rows, d), F32),
                pltpu.VMEM((items, rows, d), F32),
                pltpu.VMEM((items, rows, d), F32),
                pltpu.VMEM((rows, d_model), F32),
                pltpu.SemaphoreType.DMA((8,)),
                pltpu.SemaphoreType.DMA((items, 3)),
                pltpu.SemaphoreType.DMA((items, 3)),
                pltpu.SemaphoreType.DMA((items, 3)),
                pltpu.SemaphoreType.DMA((items, 3)),
            ],
            compiler_params=pltpu.CompilerParams(
                collective_id=0, has_side_effects=True,
                vmem_limit_bytes=50 * 1024 * 1024),
        )(*(pltpu.with_memory_space_constraint(a, pltpu.HBM) for a in (x_loc, dy_loc, w_q, w_k, w_v, w_o)))
        return pl.pallas_call(
            write_out,
            out_shape=(out, out),
            in_specs=[pl.BlockSpec(memory_space=pl.ANY)] * 2,
            out_specs=(hbm, hbm),
            scratch_shapes=[pltpu.SemaphoreType.DMA((2,))],
            compiler_params=pltpu.CompilerParams(vmem_limit_bytes=4 * 1024 * 1024),
        )(y_v, dx_v)

    return jax.shard_map(local_body, mesh=mesh,
                         in_specs=(row_spec, row_spec, full_spec, full_spec, full_spec, full_spec),
                         out_specs=(row_spec, row_spec), check_vma=False)
```

```python
import functools
import math

import jax
import jax.numpy as jnp
from jax import lax
from jax.experimental import pallas as pl
from jax.experimental.pallas import tpu as pltpu
from jax.sharding import PartitionSpec as P

HEAD_DIM = 128
CHUNK = 128
SPLIT = 128
MESH = pl.DeviceIdType.MESH
F32 = jnp.float32
BF16 = jnp.bfloat16
NT = (((1,), (1,)), ((), ()))
NN = (((1,), (0,)), ((), ()))


def mm(a, b, dims=NN):
    return lax.dot_general(a, b, dims, preferred_element_type=F32)


def kernel(rows, d_model, q_heads, kv_heads,
           x_hbm, dy_hbm, wq_hbm, wk_hbm, wv_hbm, wo_hbm,
           y_v, dx_v,
           x_v, dy_v, wq_v, wk_v, wv_v, wo_v,
           qs, dot_v, k_all, v_all, kt, vt, pt, ds_t, e_buf, m_buf, l_buf, f_buf, o_v, dq_v,
           part, recv_a, recv_b, recv_c, send_c, dx_acc,
           in_sem, ag_send, ag_recv, rs_send, rs_recv):
    group = q_heads // kv_heads
    d = HEAD_DIM
    n_keys = 4 * rows
    half = group * rows
    scale = d ** -0.5
    gain = scale * math.log2(math.e)

    me = lax.axis_index("cp")
    core = lax.rem(me, 2)
    partner = me + 1 - 2 * core
    cross = lax.rem(me + 2, 4)

    barrier = pltpu.get_barrier_semaphore()
    for peer in (partner, cross):
        pl.semaphore_signal(barrier, inc=1, device_id={"cp": peer}, device_id_type=MESH)

    qcols = q_heads * d // 2
    loads = [
        pltpu.make_async_copy(wk_hbm, wk_v, in_sem.at[1]),
        pltpu.make_async_copy(x_hbm, x_v, in_sem.at[0]),
        pltpu.make_async_copy(wv_hbm, wv_v, in_sem.at[2]),
        pltpu.make_async_copy(wq_hbm.at[:, :qcols], wq_v.at[:, :qcols], in_sem.at[3]),
        pltpu.make_async_copy(wq_hbm.at[:, qcols:], wq_v.at[:, qcols:], in_sem.at[4]),
        pltpu.make_async_copy(dy_hbm, dy_v, in_sem.at[5]),
        pltpu.make_async_copy(wo_hbm.at[:qcols], wo_v.at[:qcols], in_sem.at[6]),
        pltpu.make_async_copy(wo_hbm.at[qcols:], wo_v.at[qcols:], in_sem.at[7]),
    ]
    for copy in loads:
        copy.start()

    def item(i):
        return (k_all if i % 2 == 0 else v_all).at[i // 2]

    def slot(i, s):
        return item(i).at[pl.ds(s * rows, rows)]

    def ag_copy(i, hop):
        src, dst, peer = ((0, 1, partner), (0, 2, cross), (2, 3, partner))[hop]
        return pltpu.make_async_remote_copy(
            src_ref=slot(i, src), dst_ref=slot(i, dst),
            send_sem=ag_send.at[i, hop], recv_sem=ag_recv.at[i, hop],
            device_id={"cp": peer}, device_id_type=MESH)

    def forward(i):
        ag_copy(i, 1).wait_recv()
        ag_copy(i, 2).start()

    def transpose_item(i, ref):
        for s in range(4):
            ref[i // 2, :, s * rows:(s + 1) * rows] = slot(i, s)[...].T

    def head_of(i):
        h, j = i // group, i % group
        return h, slice(j * rows, (j + 1) * rows), slice(i * d, (i + 1) * d)

    def project_q(n):
        out = mm(x_v[...], wq_v[:, n * 2 * d:(n + 1) * 2 * d]).astype(BF16)
        for t in range(2):
            h, cols, _ = head_of(2 * n + t)
            qs[h, cols, :] = out[:, t * d:(t + 1) * d]

    def project_do(n):
        out = mm(wo_v[n * 2 * d:(n + 1) * 2 * d, :], dy_v[...], NT).astype(BF16)
        for t in range(2):
            h, cols, _ = head_of(2 * n + t)
            dot_v[h, :, cols] = out[t * d:(t + 1) * d, :]

    per_slot = rows // CHUNK

    def scores(i, s):
        h, cols, _ = head_of(i)
        j = i % group
        raw = mm(k_all[h, s * rows:(s + 1) * rows, :], qs[h, cols, :], NT)
        for c in range(per_slot):
            t = raw[c * CHUNK:(c + 1) * CHUNK] * gain
            t = t.reshape(CHUNK // 8, 8, rows)
            m8 = jnp.max(t, axis=0)
            e = jnp.exp2(t - m8[None])
            e_buf[j, s * rows + c * CHUNK:s * rows + (c + 1) * CHUNK, :] = e.reshape(CHUNK, rows)
            m_buf[j, s * per_slot + c] = m8
            l_buf[j, s * per_slot + c] = jnp.sum(e, axis=0)

    def finalize(i, slots):
        h, cols, _ = head_of(i)
        j = i % group
        n_chunks = 4 * per_slot
        if 3 in slots:
            top = jnp.max(jnp.max(m_buf[j], axis=0), axis=0, keepdims=True)
            factor = [jnp.exp2(m_buf[j, c] - top) for c in range(n_chunks)]
            total = factor[0] * l_buf[j, 0]
            for c in range(1, n_chunks):
                total = total + factor[c] * l_buf[j, c]
            inv = 1.0 / jnp.sum(total, axis=0, keepdims=True)
            for c in range(n_chunks):
                f_buf[j, c] = factor[c] * inv
        for s in slots:
            for c in range(s * per_slot, (s + 1) * per_slot):
                e = e_buf[j, c * CHUNK:(c + 1) * CHUNK, :].reshape(CHUNK // 8, 8, rows)
                pt[h, c * CHUNK:(c + 1) * CHUNK, cols] = (e * f_buf[j, c][None]).reshape(CHUNK, rows).astype(BF16)

    def outs(i):
        h, cols, feats = head_of(i)
        o_t = mm(vt[h], pt[h, :, cols]).astype(BF16)
        o_v[:, feats] = o_t.T
        do_t = dot_v[h, :, cols]
        delta = jnp.sum(do_t.astype(F32) * o_t.astype(F32), axis=0, keepdims=True)
        for s in range(4):
            keys = slice(s * rows, (s + 1) * rows)
            dp = mm(v_all[h, keys, :], do_t)
            ds_t[h, keys, cols] = (pt[h, keys, cols].astype(F32) * (dp - delta)).astype(BF16)

    def dqs(i):
        h, cols, feats = head_of(i)
        dq_v[:, feats] = (mm(kt[h], ds_t[h, :, cols]) * scale).astype(BF16).T

    def grads(r, lo, hi):
        h = r % kv_heads
        for s in range(lo, hi):
            for t in range(rows // SPLIT):
                block = slice(s * rows + t * SPLIT, s * rows + (t + 1) * SPLIT)
                if r < kv_heads:
                    out = mm(pt[h, block, :], dot_v[h], NT)
                else:
                    out = mm(ds_t[h, block, :], qs[h])
                part[r, s, t * SPLIT:(t + 1) * SPLIT, :] = out

    def rs_copy(r, kind):
        src, dst, peer = ((part.at[r, 3], recv_a.at[r], partner),
                          (part.at[r, 1], recv_b.at[r], partner),
                          (send_c.at[r], recv_c.at[r], cross))[kind]
        return pltpu.make_async_remote_copy(
            src_ref=src, dst_ref=dst,
            send_sem=rs_send.at[r, kind], recv_sem=rs_recv.at[r, kind],
            device_id={"cp": peer}, device_id_type=MESH)

    def reduce_cross(r):
        rs_copy(r, 0).wait_recv()
        send_c[r] = part[r, 2] + recv_a[r]
        rs_copy(r, 2).start()

    first = range(group)
    second = range(group, q_heads)
    n_pairs = q_heads // 4

    peers = [partner, cross]

    def stage(f):
        peers.reverse()
        pl.when(peers[0] != me)(f)

    def project_kv(w, kv_ref):
        out = mm(x_v[...], w[...]).astype(BF16)
        for h in range(kv_heads):
            kv_ref[h, :rows, :] = out[:, h * d:(h + 1) * d]

    def send_kv(item_of_head):
        for h in range(kv_heads):
            i = 2 * h + item_of_head
            ag_copy(i, 1).start()
            ag_copy(i, 0).start()

    @stage
    def _():
        loads[0].wait()
        loads[1].wait()
        project_kv(wk_v, k_all)

    pl.semaphore_wait(barrier, 2)
    send_kv(0)

    @stage
    def _():
        loads[2].wait()
        project_kv(wv_v, v_all)

    send_kv(1)

    @stage
    def _():
        loads[3].wait()
        for n in range(n_pairs):
            project_q(n)

    @stage
    def _():
        loads[4].wait()
        ag_copy(0, 0).wait_recv()
        for n in range(n_pairs):
            project_q(n_pairs + n)
            for i in (2 * n, 2 * n + 1):
                scores(i, 0)
                scores(i, 1)

    @stage
    def _():
        loads[5].wait()
        loads[6].wait()
        for n in range(n_pairs):
            project_do(n)

    @stage
    def _():
        loads[7].wait()
        forward(0)
        for n in range(n_pairs):
            project_do(n_pairs + n)
            scores(2 * n, 2)
            scores(2 * n + 1, 2)

    @stage
    def _():
        ag_copy(0, 2).wait_recv()
        for i in first:
            scores(i, 3)
        for i in first:
            finalize(i, (3, 2))

    @stage
    def _():
        forward(1)
        grads(0, 3, 4)
        rs_copy(0, 0).start()
        grads(0, 2, 3)
        for n in first:
            finalize(n, (1, 0))

    @stage
    def _():
        ag_copy(2, 0).wait_recv()
        for n in range(group):
            scores(group + n, 0)
            if n == 0:
                grads(0, 1, 2)
            if n == 3:
                grads(0, 0, 1)
            scores(group + n, 1)
        rs_copy(0, 1).start()

    @stage
    def _():
        forward(2)
        reduce_cross(0)
        ag_copy(1, 0).wait_recv()
        ag_copy(1, 2).wait_recv()
        transpose_item(1, vt)
        for i in first:
            outs(i)
            scores(group + i, 2)

    @stage
    def _():
        forward(3)
        ag_copy(2, 2).wait_recv()
        grads(2, 3, 4)
        rs_copy(2, 0).start()
        for i in second:
            scores(i, 3)
        for i in second:
            finalize(i, (3, 2))
        grads(2, 2, 3)

    @stage
    def _():
        grads(1, 3, 4)
        rs_copy(1, 0).start()
        grads(1, 2, 3)
        for i in second:
            finalize(i, (1, 0))

    @stage
    def _():
        reduce_cross(2)
        ag_copy(3, 0).wait_recv()
        ag_copy(3, 2).wait_recv()
        transpose_item(3, vt)
        for i in second[:group // 2]:
            outs(i)

    @stage
    def _():
        reduce_cross(1)
        for i in second[group // 2:]:
            outs(i)

    @stage
    def _():
        grads(3, 3, 4)
        rs_copy(3, 0).start()
        grads(3, 2, 3)
        grads(2, 0, 2)
        rs_copy(2, 1).start()
        grads(1, 0, 2)
        rs_copy(1, 1).start()

    @stage
    def _():
        reduce_cross(3)
        grads(3, 0, 2)
        rs_copy(3, 1).start()
        transpose_item(0, kt)
        transpose_item(2, kt)
        for i in range(q_heads):
            dqs(i)
        for n in range(d_model // 256):
            cols = slice(n * 256, (n + 1) * 256)
            y_v[:, cols] = mm(o_v[...], wo_v[:, cols]).astype(BF16)
        for n in range(d_model // 256):
            cols = slice(n * 256, (n + 1) * 256)
            dx_acc[:, cols] = mm(dq_v[...], wq_v[cols, :], NT)

    def own(r):
        rs_copy(r, 1).wait_recv()
        rs_copy(r, 2).wait_recv()
        total = part[r, 0] + recv_b[r] + recv_c[r]
        if r >= kv_heads:
            total = total * scale
        return total.astype(BF16)

    def add_own(r, g):
        h = r % kv_heads
        w = wv_v if r < kv_heads else wk_v
        for n in range(d_model // 256):
            cols = slice(n * 256, (n + 1) * 256)
            yield cols, dx_acc[:, cols] + mm(g, w[cols, h * d:(h + 1) * d], NT)

    for r in (0, 2, 1):
        @stage
        def _(r=r):
            for cols, total in add_own(r, own(r)):
                dx_acc[:, cols] = total

    for i in range(2 * kv_heads):
        for hop in range(3):
            ag_copy(i, hop).wait_send()
    for r in range(2 * kv_heads):
        for kind in range(3):
            if (r, kind) != (3, 2):
                rs_copy(r, kind).wait_send()

    @stage
    def _():
        for cols, total in add_own(3, own(3)):
            dx_v[:, cols] = total.astype(BF16)

    rs_copy(3, 2).wait_send()


def write_out(y_v, dx_v, y_hbm, dx_hbm, sem):
    copies = [pltpu.make_async_copy(y_v, y_hbm, sem.at[0]),
              pltpu.make_async_copy(dx_v, dx_hbm, sem.at[1])]
    for copy in copies:
        copy.start()
    for copy in copies:
        copy.wait()


def solution(mesh):
    row_spec = P(("dp", "cp"), None)
    full_spec = P(None, None)

    def local_body(x_loc, dy_loc, w_q, w_k, w_v, w_o):
        rows, d_model = x_loc.shape
        d = HEAD_DIM
        q_heads = w_q.shape[1] // d
        kv_heads = w_k.shape[1] // d
        group = q_heads // kv_heads
        n_keys = 4 * rows
        qw = q_heads * d
        hbm = pl.BlockSpec(memory_space=pltpu.HBM)
        vmem = pl.BlockSpec(memory_space=pltpu.VMEM)
        out = jax.ShapeDtypeStruct((rows, d_model), BF16)
        items = 2 * kv_heads
        y_v, dx_v = pl.pallas_call(
            functools.partial(kernel, rows, d_model, q_heads, kv_heads),
            out_shape=(out, out),
            in_specs=[hbm] * 6,
            out_specs=(vmem, vmem),
            scratch_shapes=[
                pltpu.VMEM((rows, d_model), BF16),
                pltpu.VMEM((rows, d_model), BF16),
                pltpu.VMEM((d_model, qw), BF16),
                pltpu.VMEM((d_model, kv_heads * d), BF16),
                pltpu.VMEM((d_model, kv_heads * d), BF16),
                pltpu.VMEM((qw, d_model), BF16),
                pltpu.VMEM((kv_heads, group * rows, d), BF16),
                pltpu.VMEM((kv_heads, d, group * rows), BF16),
                pltpu.VMEM((kv_heads, n_keys, d), BF16),
                pltpu.VMEM((kv_heads, n_keys, d), BF16),
                pltpu.VMEM((kv_heads, d, n_keys), BF16),
                pltpu.VMEM((kv_heads, d, n_keys), BF16),
                pltpu.VMEM((kv_heads, n_keys, group * rows), BF16),
                pltpu.VMEM((kv_heads, n_keys, group * rows), BF16),
                pltpu.VMEM((group, n_keys, rows), F32),
                pltpu.VMEM((group, n_keys // CHUNK, 8, rows), F32),
                pltpu.VMEM((group, n_keys // CHUNK, 8, rows), F32),
                pltpu.VMEM((group, n_keys // CHUNK, 8, rows), F32),
                pltpu.VMEM((rows, qw), BF16),
                pltpu.VMEM((rows, qw), BF16),
                pltpu.VMEM((items, 4, rows, d), F32),
                pltpu.VMEM((items, rows, d), F32),
                pltpu.VMEM((items, rows, d), F32),
                pltpu.VMEM((items, rows, d), F32),
                pltpu.VMEM((items, rows, d), F32),
                pltpu.VMEM((rows, d_model), F32),
                pltpu.SemaphoreType.DMA((8,)),
                pltpu.SemaphoreType.DMA((items, 3)),
                pltpu.SemaphoreType.DMA((items, 3)),
                pltpu.SemaphoreType.DMA((items, 3)),
                pltpu.SemaphoreType.DMA((items, 3)),
            ],
            compiler_params=pltpu.CompilerParams(
                collective_id=0, has_side_effects=True,
                vmem_limit_bytes=50 * 1024 * 1024),
        )(*(pltpu.with_memory_space_constraint(a, pltpu.HBM) for a in (x_loc, dy_loc, w_q, w_k, w_v, w_o)))
        return pl.pallas_call(
            write_out,
            out_shape=(out, out),
            in_specs=[pl.BlockSpec(memory_space=pl.ANY)] * 2,
            out_specs=(hbm, hbm),
            scratch_shapes=[pltpu.SemaphoreType.DMA((2,))],
            compiler_params=pltpu.CompilerParams(vmem_limit_bytes=4 * 1024 * 1024),
        )(y_v, dx_v)

    return jax.shard_map(local_body, mesh=mesh,
                         in_specs=(row_spec, row_spec, full_spec, full_spec, full_spec, full_spec),
                         out_specs=(row_spec, row_spec), check_vma=False)
```

```python
import functools
import math

import jax
import jax.numpy as jnp
from jax import lax
from jax.experimental import pallas as pl
from jax.experimental.pallas import tpu as pltpu
from jax.sharding import PartitionSpec as P

HEAD_DIM = 128
CHUNK = 128
SPLIT = 128
MESH = pl.DeviceIdType.MESH
F32 = jnp.float32
BF16 = jnp.bfloat16
NT = (((1,), (1,)), ((), ()))
NN = (((1,), (0,)), ((), ()))


def mm(a, b, dims=NN):
    return lax.dot_general(a, b, dims, preferred_element_type=F32)


def kernel(rows, d_model, q_heads, kv_heads,
           x_hbm, dy_hbm, wq_hbm, wk_hbm, wv_hbm, wo_hbm,
           y_v, dx_v,
           x_v, dy_v, wq_v, wk_v, wv_v, wo_v,
           qs, dot_v, k_all, v_all, kt, vt, pt, ds_t, e_buf, m_buf, l_buf, f_buf, o_v, dq_v,
           part, recv_a, recv_b, recv_c, send_c, dx_acc,
           in_sem, ag_send, ag_recv, rs_send, rs_recv):
    group = q_heads // kv_heads
    d = HEAD_DIM
    n_keys = 4 * rows
    half = group * rows
    scale = d ** -0.5
    gain = scale * math.log2(math.e)

    me = lax.axis_index("cp")
    core = lax.rem(me, 2)
    partner = me + 1 - 2 * core
    cross = lax.rem(me + 2, 4)

    barrier = pltpu.get_barrier_semaphore()
    for peer in (partner, cross):
        pl.semaphore_signal(barrier, inc=1, device_id={"cp": peer}, device_id_type=MESH)

    qcols = q_heads * d // 2
    loads = [
        pltpu.make_async_copy(wk_hbm, wk_v, in_sem.at[1]),
        pltpu.make_async_copy(x_hbm, x_v, in_sem.at[0]),
        pltpu.make_async_copy(wv_hbm, wv_v, in_sem.at[2]),
        pltpu.make_async_copy(wq_hbm.at[:, :qcols], wq_v.at[:, :qcols], in_sem.at[3]),
        pltpu.make_async_copy(wq_hbm.at[:, qcols:], wq_v.at[:, qcols:], in_sem.at[4]),
        pltpu.make_async_copy(dy_hbm, dy_v, in_sem.at[5]),
        pltpu.make_async_copy(wo_hbm.at[:qcols], wo_v.at[:qcols], in_sem.at[6]),
        pltpu.make_async_copy(wo_hbm.at[qcols:], wo_v.at[qcols:], in_sem.at[7]),
    ]
    for copy in loads:
        copy.start()

    def item(i):
        return (k_all if i % 2 == 0 else v_all).at[i // 2]

    def slot(i, s):
        return item(i).at[pl.ds(s * rows, rows)]

    def ag_copy(i, hop):
        src, dst, peer = ((0, 1, partner), (0, 2, cross), (2, 3, partner))[hop]
        return pltpu.make_async_remote_copy(
            src_ref=slot(i, src), dst_ref=slot(i, dst),
            send_sem=ag_send, recv_sem=ag_recv.at[i, hop],
            device_id={"cp": peer}, device_id_type=MESH)

    def forward(i):
        ag_copy(i, 1).wait_recv()
        ag_copy(i, 2).start()

    def transpose_item(i, ref):
        for s in range(4):
            ref[i // 2, :, s * rows:(s + 1) * rows] = slot(i, s)[...].T

    def head_of(i):
        h, j = i // group, i % group
        return h, slice(j * rows, (j + 1) * rows), slice(i * d, (i + 1) * d)

    def project_q(n):
        out = mm(x_v[...], wq_v[:, n * 2 * d:(n + 1) * 2 * d]).astype(BF16)
        for t in range(2):
            h, cols, _ = head_of(2 * n + t)
            qs[h, cols, :] = out[:, t * d:(t + 1) * d]

    def project_do(n):
        out = mm(wo_v[n * 2 * d:(n + 1) * 2 * d, :], dy_v[...], NT).astype(BF16)
        for t in range(2):
            h, cols, _ = head_of(2 * n + t)
            dot_v[h, :, cols] = out[t * d:(t + 1) * d, :]

    per_slot = rows // CHUNK

    def scores(i, s):
        h, cols, _ = head_of(i)
        j = i
        raw = mm(k_all[h, s * rows:(s + 1) * rows, :], qs[h, cols, :], NT)
        for c in range(per_slot):
            t = raw[c * CHUNK:(c + 1) * CHUNK] * gain
            t = t.reshape(CHUNK // 8, 8, rows)
            m8 = jnp.max(t, axis=0)
            e = jnp.exp2(t - m8[None])
            e_buf[j, s * rows + c * CHUNK:s * rows + (c + 1) * CHUNK, :] = e.reshape(CHUNK, rows)
            m_buf[j, s * per_slot + c] = m8
            l_buf[j, s * per_slot + c] = jnp.sum(e, axis=0)

    def finalize(i, slots):
        h, cols, _ = head_of(i)
        j = i
        n_chunks = 4 * per_slot
        if 3 in slots:
            top = jnp.max(jnp.max(m_buf[j], axis=0), axis=0, keepdims=True)
            factor = [jnp.exp2(m_buf[j, c] - top) for c in range(n_chunks)]
            total = factor[0] * l_buf[j, 0]
            for c in range(1, n_chunks):
                total = total + factor[c] * l_buf[j, c]
            inv = 1.0 / jnp.sum(total, axis=0, keepdims=True)
            for c in range(n_chunks):
                f_buf[j, c] = factor[c] * inv
        for s in slots:
            for c in range(s * per_slot, (s + 1) * per_slot):
                e = e_buf[j, c * CHUNK:(c + 1) * CHUNK, :].reshape(CHUNK // 8, 8, rows)
                pt[h, c * CHUNK:(c + 1) * CHUNK, cols] = (e * f_buf[j, c][None]).reshape(CHUNK, rows).astype(BF16)

    def out_head(i):
        h, cols, feats = head_of(i)
        o_t = mm(vt[h], pt[h, :, cols]).astype(BF16)
        o_v[:, feats] = o_t.T
        return jnp.sum(dot_v[h, :, cols].astype(F32) * o_t.astype(F32), axis=0, keepdims=True)

    def dscore(i, delta):
        h, cols, _ = head_of(i)
        do_t = dot_v[h, :, cols]
        for s in range(4):
            keys = slice(s * rows, (s + 1) * rows)
            dp = mm(v_all[h, keys, :], do_t)
            ds_t[h, keys, cols] = (pt[h, keys, cols].astype(F32) * (dp - delta)).astype(BF16)

    def out_all(heads):
        heads = list(heads)
        delta = out_head(heads[0])
        for i, after in zip(heads, heads[1:] + [None]):
            delta_after = None if after is None else out_head(after)
            dscore(i, delta)
            delta = delta_after

    def dqs(i):
        h, cols, feats = head_of(i)
        dq_v[:, feats] = (mm(kt[h], ds_t[h, :, cols]) * scale).astype(BF16).T

    def grads(r, lo, hi):
        h = r % kv_heads
        for s in range(lo, hi):
            for t in range(rows // SPLIT):
                block = slice(s * rows + t * SPLIT, s * rows + (t + 1) * SPLIT)
                if r < kv_heads:
                    out = mm(pt[h, block, :], dot_v[h], NT)
                else:
                    out = mm(ds_t[h, block, :], qs[h])
                part[r, s, t * SPLIT:(t + 1) * SPLIT, :] = out

    def rs_copy(r, kind):
        src, dst, peer = ((part.at[r, 3], recv_a.at[r], partner),
                          (part.at[r, 1], recv_b.at[r], partner),
                          (send_c.at[r], recv_c.at[r], cross))[kind]
        return pltpu.make_async_remote_copy(
            src_ref=src, dst_ref=dst,
            send_sem=rs_send, recv_sem=rs_recv.at[r, kind],
            device_id={"cp": peer}, device_id_type=MESH)

    def reduce_cross(r):
        rs_copy(r, 0).wait_recv()
        send_c[r] = part[r, 2] + recv_a[r]
        rs_copy(r, 2).start()

    first = range(group)
    second = range(group, q_heads)
    n_pairs = q_heads // 4

    peers = [partner, cross]

    def stage(f):
        peers.reverse()
        pl.when(peers[0] != me)(f)

    def project_kv(w, kv_ref):
        out = mm(x_v[...], w[...]).astype(BF16)
        for h in range(kv_heads):
            kv_ref[h, :rows, :] = out[:, h * d:(h + 1) * d]

    def send_kv(item_of_head):
        for h in range(kv_heads):
            i = 2 * h + item_of_head
            ag_copy(i, 1).start()
            ag_copy(i, 0).start()

    @stage
    def _():
        loads[0].wait()
        loads[1].wait()
        project_kv(wk_v, k_all)

    pl.semaphore_wait(barrier, 2)
    send_kv(0)

    @stage
    def _():
        loads[2].wait()
        project_kv(wv_v, v_all)

    send_kv(1)

    @stage
    def _():
        loads[3].wait()
        for n in range(n_pairs):
            project_q(n)

    @stage
    def _():
        loads[4].wait()
        ag_copy(0, 0).wait_recv()
        for n in range(n_pairs):
            project_q(n_pairs + n)
            for i in (2 * n, 2 * n + 1):
                scores(i, 0)
                scores(i, 1)

    @stage
    def _():
        loads[5].wait()
        loads[6].wait()
        ag_copy(2, 0).wait_recv()
        for n in range(n_pairs):
            project_do(n)
            for i in (2 * n, 2 * n + 1):
                scores(group + i, 0)
                scores(group + i, 1)

    @stage
    def _():
        loads[7].wait()
        forward(0)
        for n in range(n_pairs):
            if n == 0:
                project_do(n_pairs)
            scores(2 * n, 2)
            scores(2 * n + 1, 2)

    @stage
    def _():
        ag_copy(0, 2).wait_recv()
        for n in range(n_pairs):
            scores(2 * n, 3)
            scores(2 * n + 1, 3)
            if n > 0:
                project_do(n_pairs + n)
            finalize(2 * n, (3, 2))
            finalize(2 * n + 1, (3, 2))

    @stage
    def _():
        forward(1)
        grads(0, 3, 4)
        grads(0, 2, 3)
        for n in first:
            finalize(n, (1, 0))
        rs_copy(0, 0).start()

    @stage
    def _():
        forward(2)
        for n in range(group):
            scores(group + n, 2)
            if n == 1:
                grads(0, 1, 2)
            if n == 3:
                grads(0, 0, 1)
        rs_copy(0, 1).start()

    @stage
    def _():
        reduce_cross(0)
        ag_copy(1, 0).wait_recv()
        ag_copy(1, 2).wait_recv()
        transpose_item(1, vt)
        out_all(first)

    @stage
    def _():
        forward(3)
        ag_copy(2, 2).wait_recv()
        for n in range(n_pairs):
            scores(group + 2 * n, 3)
            scores(group + 2 * n + 1, 3)
            if n > 0:
                grads(2, 4 - n, 5 - n)
            finalize(group + 2 * n, (3, 2))
            finalize(group + 2 * n + 1, (3, 2))
        rs_copy(2, 0).start()

    @stage
    def _():
        grads(1, 3, 4)
        grads(1, 2, 3)
        for i in second:
            finalize(i, (1, 0))
        rs_copy(1, 0).start()

    @stage
    def _():
        ag_copy(3, 0).wait_recv()
        ag_copy(3, 2).wait_recv()
        transpose_item(3, vt)
        out_all(second[:group // 2])
        grads(2, 0, 2)
        rs_copy(2, 1).start()

    @stage
    def _():
        reduce_cross(2)
        out_all(second[group // 2:])

    @stage
    def _():
        reduce_cross(1)
        grads(3, 3, 4)
        grads(3, 2, 3)
        grads(1, 0, 2)
        rs_copy(3, 0).start()
        rs_copy(1, 1).start()

    @stage
    def _():
        grads(3, 0, 2)
        transpose_item(0, kt)
        for i in first:
            dqs(i)
        transpose_item(2, kt)
        for i in second:
            dqs(i)
        rs_copy(3, 1).start()

    @stage
    def _():
        reduce_cross(3)
        for n in range(d_model // 256):
            cols = slice(n * 256, (n + 1) * 256)
            y_v[:, cols] = mm(o_v[...], wo_v[:, cols]).astype(BF16)

    def own(items, factor):
        parts = []
        for r in items:
            rs_copy(r, 1).wait_recv()
            rs_copy(r, 2).wait_recv()
        for r in items:
            total = part[r, 0] + recv_b[r] + recv_c[r]
            parts.append((total * factor).astype(BF16) if factor != 1 else total.astype(BF16))
        return jnp.concatenate(parts, axis=1)

    @stage
    def _():
        dv = own((0, 1), 1)
        for n in range(d_model // 256):
            cols = slice(n * 256, (n + 1) * 256)
            dx_acc[:, cols] = mm(dq_v[...], wq_v[cols, :], NT) + mm(dv, wv_v[cols, :], NT)

    pltpu.make_async_copy(x_v, x_v, ag_send).wait()

    @stage
    def _():
        dk = own((2, 3), scale)
        for n in range(d_model // 256):
            cols = slice(n * 256, (n + 1) * 256)
            dx_v[:, cols] = (dx_acc[:, cols] + mm(dk, wk_v[cols, :], NT)).astype(BF16)

    pltpu.make_async_copy(dx_acc, dx_acc, rs_send).wait()


def write_out(y_v, dx_v, y_hbm, dx_hbm, sem):
    copies = [pltpu.make_async_copy(y_v, y_hbm, sem.at[0]),
              pltpu.make_async_copy(dx_v, dx_hbm, sem.at[1])]
    for copy in copies:
        copy.start()
    for copy in copies:
        copy.wait()


def solution(mesh):
    row_spec = P(("dp", "cp"), None)
    full_spec = P(None, None)

    def local_body(x_loc, dy_loc, w_q, w_k, w_v, w_o):
        rows, d_model = x_loc.shape
        d = HEAD_DIM
        q_heads = w_q.shape[1] // d
        kv_heads = w_k.shape[1] // d
        group = q_heads // kv_heads
        n_keys = 4 * rows
        qw = q_heads * d
        hbm = pl.BlockSpec(memory_space=pltpu.HBM)
        vmem = pl.BlockSpec(memory_space=pltpu.VMEM)
        out = jax.ShapeDtypeStruct((rows, d_model), BF16)
        items = 2 * kv_heads
        y_v, dx_v = pl.pallas_call(
            functools.partial(kernel, rows, d_model, q_heads, kv_heads),
            out_shape=(out, out),
            in_specs=[hbm] * 6,
            out_specs=(vmem, vmem),
            scratch_shapes=[
                pltpu.VMEM((rows, d_model), BF16),
                pltpu.VMEM((rows, d_model), BF16),
                pltpu.VMEM((d_model, qw), BF16),
                pltpu.VMEM((d_model, kv_heads * d), BF16),
                pltpu.VMEM((d_model, kv_heads * d), BF16),
                pltpu.VMEM((qw, d_model), BF16),
                pltpu.VMEM((kv_heads, group * rows, d), BF16),
                pltpu.VMEM((kv_heads, d, group * rows), BF16),
                pltpu.VMEM((kv_heads, n_keys, d), BF16),
                pltpu.VMEM((kv_heads, n_keys, d), BF16),
                pltpu.VMEM((kv_heads, d, n_keys), BF16),
                pltpu.VMEM((kv_heads, d, n_keys), BF16),
                pltpu.VMEM((kv_heads, n_keys, group * rows), BF16),
                pltpu.VMEM((kv_heads, n_keys, group * rows), BF16),
                pltpu.VMEM((q_heads, n_keys, rows), F32),
                pltpu.VMEM((q_heads, n_keys // CHUNK, 8, rows), F32),
                pltpu.VMEM((q_heads, n_keys // CHUNK, 8, rows), F32),
                pltpu.VMEM((q_heads, n_keys // CHUNK, 8, rows), F32),
                pltpu.VMEM((rows, qw), BF16),
                pltpu.VMEM((rows, qw), BF16),
                pltpu.VMEM((items, 4, rows, d), F32),
                pltpu.VMEM((items, rows, d), F32),
                pltpu.VMEM((items, rows, d), F32),
                pltpu.VMEM((items, rows, d), F32),
                pltpu.VMEM((items, rows, d), F32),
                pltpu.VMEM((rows, d_model), F32),
                pltpu.SemaphoreType.DMA((8,)),
                pltpu.SemaphoreType.DMA,
                pltpu.SemaphoreType.DMA((items, 3)),
                pltpu.SemaphoreType.DMA,
                pltpu.SemaphoreType.DMA((items, 3)),
            ],
            compiler_params=pltpu.CompilerParams(
                collective_id=0, has_side_effects=True,
                vmem_limit_bytes=52 * 1024 * 1024),
        )(*(pltpu.with_memory_space_constraint(a, pltpu.HBM) for a in (x_loc, dy_loc, w_q, w_k, w_v, w_o)))
        return pl.pallas_call(
            write_out,
            out_shape=(out, out),
            in_specs=[pl.BlockSpec(memory_space=pl.ANY)] * 2,
            out_specs=(hbm, hbm),
            scratch_shapes=[pltpu.SemaphoreType.DMA((2,))],
            compiler_params=pltpu.CompilerParams(vmem_limit_bytes=4 * 1024 * 1024),
        )(y_v, dx_v)

    return jax.shard_map(local_body, mesh=mesh,
                         in_specs=(row_spec, row_spec, full_spec, full_spec, full_spec, full_spec),
                         out_specs=(row_spec, row_spec), check_vma=False)
```

```python
import functools
import math

import jax
import jax.numpy as jnp
from jax import lax
from jax.experimental import pallas as pl
from jax.experimental.pallas import tpu as pltpu
from jax.sharding import PartitionSpec as P

HEAD_DIM = 128
CHUNK = 128
SPLIT = 128
MESH = pl.DeviceIdType.MESH
F32 = jnp.float32
BF16 = jnp.bfloat16
NT = (((1,), (1,)), ((), ()))
NN = (((1,), (0,)), ((), ()))


def mm(a, b, dims=NN):
    return lax.dot_general(a, b, dims, preferred_element_type=F32)


def kernel(rows, d_model, q_heads, kv_heads,
           x_hbm, dy_hbm, wq_hbm, wk_hbm, wv_hbm, wo_hbm,
           y_v, dx_v,
           x_v, dy_v, wq_v, wk_v, wv_v, wo_v,
           qs, dot_v, k_all, v_all, kt, vt, pt, ds_t, e_buf, m_buf, l_buf, f_buf, o_v, dq_v,
           part, recv_a, recv_b, recv_c, send_c, dx_acc,
           in_sem, ag_send, ag_recv, rs_send, rs_recv):
    group = q_heads // kv_heads
    d = HEAD_DIM
    n_keys = 4 * rows
    half = group * rows
    scale = d ** -0.5
    gain = scale * math.log2(math.e)

    me = lax.axis_index("cp")
    core = lax.rem(me, 2)
    partner = me + 1 - 2 * core
    cross = lax.rem(me + 2, 4)

    barrier = pltpu.get_barrier_semaphore()
    for peer in (partner, cross):
        pl.semaphore_signal(barrier, inc=1, device_id={"cp": peer}, device_id_type=MESH)

    qcols = q_heads * d // 2
    loads = [
        pltpu.make_async_copy(wk_hbm, wk_v, in_sem.at[1]),
        pltpu.make_async_copy(x_hbm, x_v, in_sem.at[0]),
        pltpu.make_async_copy(wv_hbm, wv_v, in_sem.at[2]),
        pltpu.make_async_copy(wq_hbm.at[:, :qcols], wq_v.at[:, :qcols], in_sem.at[3]),
        pltpu.make_async_copy(wq_hbm.at[:, qcols:], wq_v.at[:, qcols:], in_sem.at[4]),
        pltpu.make_async_copy(dy_hbm, dy_v, in_sem.at[5]),
        pltpu.make_async_copy(wo_hbm.at[:qcols], wo_v.at[:qcols], in_sem.at[6]),
        pltpu.make_async_copy(wo_hbm.at[qcols:], wo_v.at[qcols:], in_sem.at[7]),
    ]
    for copy in loads:
        copy.start()

    def item(i):
        return (k_all if i % 2 == 0 else v_all).at[i // 2]

    def slot(i, s):
        return item(i).at[pl.ds(s * rows, rows)]

    def ag_copy(i, hop):
        src, dst, peer = ((0, 1, partner), (0, 2, cross), (2, 3, partner))[hop]
        return pltpu.make_async_remote_copy(
            src_ref=slot(i, src), dst_ref=slot(i, dst),
            send_sem=ag_send, recv_sem=ag_recv.at[i, hop],
            device_id={"cp": peer}, device_id_type=MESH)

    def forward(i):
        ag_copy(i, 1).wait_recv()
        ag_copy(i, 2).start()

    def transpose_item(i, ref):
        for s in range(4):
            ref[i // 2, :, s * rows:(s + 1) * rows] = slot(i, s)[...].T

    def head_of(i):
        h, j = i // group, i % group
        return h, slice(j * rows, (j + 1) * rows), slice(i * d, (i + 1) * d)

    def project_q(n):
        out = mm(x_v[...], wq_v[:, n * 2 * d:(n + 1) * 2 * d]).astype(BF16)
        for t in range(2):
            h, cols, _ = head_of(2 * n + t)
            qs[h, cols, :] = out[:, t * d:(t + 1) * d]

    def project_do(n):
        out = mm(wo_v[n * 2 * d:(n + 1) * 2 * d, :], dy_v[...], NT).astype(BF16)
        for t in range(2):
            h, cols, _ = head_of(2 * n + t)
            dot_v[h, :, cols] = out[t * d:(t + 1) * d, :]

    per_slot = rows // CHUNK

    def scores(i, s):
        h, cols, _ = head_of(i)
        j = i
        raw = mm(k_all[h, s * rows:(s + 1) * rows, :], qs[h, cols, :], NT)
        for c in range(per_slot):
            t = raw[c * CHUNK:(c + 1) * CHUNK] * gain
            t = t.reshape(CHUNK // 8, 8, rows)
            m8 = jnp.max(t, axis=0)
            e = jnp.exp2(t - m8[None])
            e_buf[j, s * rows + c * CHUNK:s * rows + (c + 1) * CHUNK, :] = e.reshape(CHUNK, rows)
            m_buf[j, s * per_slot + c] = m8
            l_buf[j, s * per_slot + c] = jnp.sum(e, axis=0)

    def finalize(i, slots):
        h, cols, _ = head_of(i)
        j = i
        n_chunks = 4 * per_slot
        if 3 in slots:
            top = jnp.max(jnp.max(m_buf[j], axis=0), axis=0, keepdims=True)
            factor = [jnp.exp2(m_buf[j, c] - top) for c in range(n_chunks)]
            total = factor[0] * l_buf[j, 0]
            for c in range(1, n_chunks):
                total = total + factor[c] * l_buf[j, c]
            inv = 1.0 / jnp.sum(total, axis=0, keepdims=True)
            for c in range(n_chunks):
                f_buf[j, c] = factor[c] * inv
        for s in slots:
            for c in range(s * per_slot, (s + 1) * per_slot):
                e = e_buf[j, c * CHUNK:(c + 1) * CHUNK, :].reshape(CHUNK // 8, 8, rows)
                pt[h, c * CHUNK:(c + 1) * CHUNK, cols] = (e * f_buf[j, c][None]).reshape(CHUNK, rows).astype(BF16)

    def out_head(i):
        h, cols, feats = head_of(i)
        o_t = mm(vt[h], pt[h, :, cols]).astype(BF16)
        o_v[:, feats] = o_t.T
        return jnp.sum(dot_v[h, :, cols].astype(F32) * o_t.astype(F32), axis=0, keepdims=True)

    def dscore(i, delta):
        h, cols, _ = head_of(i)
        do_t = dot_v[h, :, cols]
        for s in range(4):
            keys = slice(s * rows, (s + 1) * rows)
            dp = mm(v_all[h, keys, :], do_t)
            ds_t[h, keys, cols] = (pt[h, keys, cols].astype(F32) * (dp - delta)).astype(BF16)

    def out_all(heads):
        heads = list(heads)
        delta = out_head(heads[0])
        for i, after in zip(heads, heads[1:] + [None]):
            delta_after = None if after is None else out_head(after)
            dscore(i, delta)
            delta = delta_after

    def dqs(i):
        h, cols, feats = head_of(i)
        dq_v[:, feats] = (mm(kt[h], ds_t[h, :, cols]) * scale).astype(BF16).T

    def grads(r, lo, hi):
        h = r % kv_heads
        for s in range(lo, hi):
            for t in range(rows // SPLIT):
                block = slice(s * rows + t * SPLIT, s * rows + (t + 1) * SPLIT)
                if r < kv_heads:
                    out = mm(pt[h, block, :], dot_v[h], NT)
                else:
                    out = mm(ds_t[h, block, :], qs[h])
                part[r, s, t * SPLIT:(t + 1) * SPLIT, :] = out

    def rs_copy(r, kind):
        src, dst, peer = ((part.at[r, 3], recv_a.at[r], partner),
                          (part.at[r, 1], recv_b.at[r], partner),
                          (send_c.at[r], recv_c.at[r], cross))[kind]
        return pltpu.make_async_remote_copy(
            src_ref=src, dst_ref=dst,
            send_sem=rs_send, recv_sem=rs_recv.at[r, kind],
            device_id={"cp": peer}, device_id_type=MESH)

    def reduce_cross(r):
        rs_copy(r, 0).wait_recv()
        send_c[r] = part[r, 2] + recv_a[r]
        rs_copy(r, 2).start()

    first = range(group)
    second = range(group, q_heads)
    n_pairs = q_heads // 4

    peers = [partner, cross]

    def stage(f):
        peers.reverse()
        pl.when(peers[0] != me)(f)

    def project_kv(w, kv_ref):
        out = mm(x_v[...], w[...]).astype(BF16)
        for h in range(kv_heads):
            kv_ref[h, :rows, :] = out[:, h * d:(h + 1) * d]

    def send_kv(item_of_head):
        for h in range(kv_heads):
            i = 2 * h + item_of_head
            ag_copy(i, 1).start()
            ag_copy(i, 0).start()

    @stage
    def _():
        loads[0].wait()
        loads[1].wait()
        project_kv(wk_v, k_all)

    pl.semaphore_wait(barrier, 2)
    send_kv(0)

    @stage
    def _():
        loads[2].wait()
        project_kv(wv_v, v_all)

    send_kv(1)

    @stage
    def _():
        loads[3].wait()
        for n in range(n_pairs):
            project_q(n)

    @stage
    def _():
        loads[4].wait()
        ag_copy(0, 0).wait_recv()
        for n in range(n_pairs):
            project_q(n_pairs + n)
            for i in (2 * n, 2 * n + 1):
                scores(i, 0)
                scores(i, 1)

    @stage
    def _():
        loads[5].wait()
        loads[6].wait()
        ag_copy(2, 0).wait_recv()
        for n in range(n_pairs):
            project_do(n)
            scores(group + n, 0)
            scores(group + n, 1)

    @stage
    def _():
        loads[7].wait()
        forward(0)
        project_do(n_pairs)
        for n in range(n_pairs):
            scores(group + n_pairs + n, 0)
            scores(group + n_pairs + n, 1)

    @stage
    def _():
        for n in range(n_pairs):
            if n > 0:
                project_do(n_pairs + n)
            scores(2 * n, 2)
            scores(2 * n + 1, 2)

    @stage
    def _():
        ag_copy(0, 2).wait_recv()
        for n in range(n_pairs):
            scores(2 * n, 3)
            scores(2 * n + 1, 3)
            finalize(2 * n, (3, 2))
            finalize(2 * n + 1, (3, 2))

    @stage
    def _():
        forward(1)
        grads(0, 3, 4)
        rs_copy(0, 0).start()

    @stage
    def _():
        grads(0, 2, 3)
        for n in first:
            finalize(n, (1, 0))

    @stage
    def _():
        forward(2)
        for n in range(group):
            scores(group + n, 2)
            if n == 1:
                grads(0, 1, 2)

    @stage
    def _():
        reduce_cross(0)
        rs_copy(0, 1).start()
        ag_copy(2, 2).wait_recv()
        for n in range(n_pairs):
            scores(group + 2 * n, 3)
            scores(group + 2 * n + 1, 3)
            if n == 1:
                grads(0, 0, 1)
            finalize(group + 2 * n, (3, 2))
            finalize(group + 2 * n + 1, (3, 2))

    @stage
    def _():
        forward(3)
        grads(1, 3, 4)
        rs_copy(1, 0).start()

    @stage
    def _():
        ag_copy(1, 0).wait_recv()
        ag_copy(1, 2).wait_recv()
        transpose_item(1, vt)
        grads(1, 2, 3)
        for i in second:
            finalize(i, (1, 0))

    @stage
    def _():
        out_all(first[:group // 2])

    @stage
    def _():
        reduce_cross(1)
        out_all(first[group // 2:])

    @stage
    def _():
        grads(2, 3, 4)
        rs_copy(2, 0).start()

    @stage
    def _():
        ag_copy(3, 0).wait_recv()
        ag_copy(3, 2).wait_recv()
        transpose_item(3, vt)
        grads(2, 2, 3)
        out_all(second[:group // 2])

    @stage
    def _():
        reduce_cross(2)
        out_all(second[group // 2:])

    @stage
    def _():
        grads(3, 3, 4)
        rs_copy(3, 0).start()

    @stage
    def _():
        grads(3, 2, 3)
        grads(1, 0, 2)
        grads(2, 0, 2)
        grads(3, 0, 2)
        rs_copy(1, 1).start()
        rs_copy(2, 1).start()
        rs_copy(3, 1).start()

    @stage
    def _():
        reduce_cross(3)
        transpose_item(0, kt)
        for i in first:
            dqs(i)
        transpose_item(2, kt)
        for i in second:
            dqs(i)
        for n in range(d_model // 256):
            cols = slice(n * 256, (n + 1) * 256)
            y_v[:, cols] = mm(o_v[...], wo_v[:, cols]).astype(BF16)

    def own(items, factor):
        parts = []
        for r in items:
            rs_copy(r, 1).wait_recv()
            rs_copy(r, 2).wait_recv()
        for r in items:
            total = part[r, 0] + recv_b[r] + recv_c[r]
            parts.append((total * factor).astype(BF16) if factor != 1 else total.astype(BF16))
        return jnp.concatenate(parts, axis=1)

    @stage
    def _():
        dv = own((0, 1), 1)
        for n in range(d_model // 256):
            cols = slice(n * 256, (n + 1) * 256)
            dx_acc[:, cols] = mm(dq_v[...], wq_v[cols, :], NT) + mm(dv, wv_v[cols, :], NT)

    pltpu.make_async_copy(x_v, x_v, ag_send).wait()

    @stage
    def _():
        dk = own((2, 3), scale)
        for n in range(d_model // 256):
            cols = slice(n * 256, (n + 1) * 256)
            dx_v[:, cols] = (dx_acc[:, cols] + mm(dk, wk_v[cols, :], NT)).astype(BF16)

    pltpu.make_async_copy(dx_acc, dx_acc, rs_send).wait()


def write_out(y_v, dx_v, y_hbm, dx_hbm, sem):
    copies = [pltpu.make_async_copy(y_v, y_hbm, sem.at[0]),
              pltpu.make_async_copy(dx_v, dx_hbm, sem.at[1])]
    for copy in copies:
        copy.start()
    for copy in copies:
        copy.wait()


def solution(mesh):
    row_spec = P(("dp", "cp"), None)
    full_spec = P(None, None)

    def local_body(x_loc, dy_loc, w_q, w_k, w_v, w_o):
        rows, d_model = x_loc.shape
        d = HEAD_DIM
        q_heads = w_q.shape[1] // d
        kv_heads = w_k.shape[1] // d
        group = q_heads // kv_heads
        n_keys = 4 * rows
        qw = q_heads * d
        hbm = pl.BlockSpec(memory_space=pltpu.HBM)
        vmem = pl.BlockSpec(memory_space=pltpu.VMEM)
        out = jax.ShapeDtypeStruct((rows, d_model), BF16)
        items = 2 * kv_heads
        y_v, dx_v = pl.pallas_call(
            functools.partial(kernel, rows, d_model, q_heads, kv_heads),
            out_shape=(out, out),
            in_specs=[hbm] * 6,
            out_specs=(vmem, vmem),
            scratch_shapes=[
                pltpu.VMEM((rows, d_model), BF16),
                pltpu.VMEM((rows, d_model), BF16),
                pltpu.VMEM((d_model, qw), BF16),
                pltpu.VMEM((d_model, kv_heads * d), BF16),
                pltpu.VMEM((d_model, kv_heads * d), BF16),
                pltpu.VMEM((qw, d_model), BF16),
                pltpu.VMEM((kv_heads, group * rows, d), BF16),
                pltpu.VMEM((kv_heads, d, group * rows), BF16),
                pltpu.VMEM((kv_heads, n_keys, d), BF16),
                pltpu.VMEM((kv_heads, n_keys, d), BF16),
                pltpu.VMEM((kv_heads, d, n_keys), BF16),
                pltpu.VMEM((kv_heads, d, n_keys), BF16),
                pltpu.VMEM((kv_heads, n_keys, group * rows), BF16),
                pltpu.VMEM((kv_heads, n_keys, group * rows), BF16),
                pltpu.VMEM((q_heads, n_keys, rows), F32),
                pltpu.VMEM((q_heads, n_keys // CHUNK, 8, rows), F32),
                pltpu.VMEM((q_heads, n_keys // CHUNK, 8, rows), F32),
                pltpu.VMEM((q_heads, n_keys // CHUNK, 8, rows), F32),
                pltpu.VMEM((rows, qw), BF16),
                pltpu.VMEM((rows, qw), BF16),
                pltpu.VMEM((items, 4, rows, d), F32),
                pltpu.VMEM((items, rows, d), F32),
                pltpu.VMEM((items, rows, d), F32),
                pltpu.VMEM((items, rows, d), F32),
                pltpu.VMEM((items, rows, d), F32),
                pltpu.VMEM((rows, d_model), F32),
                pltpu.SemaphoreType.DMA((8,)),
                pltpu.SemaphoreType.DMA,
                pltpu.SemaphoreType.DMA((items, 3)),
                pltpu.SemaphoreType.DMA,
                pltpu.SemaphoreType.DMA((items, 3)),
            ],
            compiler_params=pltpu.CompilerParams(
                collective_id=0, has_side_effects=True,
                vmem_limit_bytes=52 * 1024 * 1024),
        )(*(pltpu.with_memory_space_constraint(a, pltpu.HBM) for a in (x_loc, dy_loc, w_q, w_k, w_v, w_o)))
        return pl.pallas_call(
            write_out,
            out_shape=(out, out),
            in_specs=[pl.BlockSpec(memory_space=pl.ANY)] * 2,
            out_specs=(hbm, hbm),
            scratch_shapes=[pltpu.SemaphoreType.DMA((2,))],
            compiler_params=pltpu.CompilerParams(vmem_limit_bytes=4 * 1024 * 1024),
        )(y_v, dx_v)

    return jax.shard_map(local_body, mesh=mesh,
                         in_specs=(row_spec, row_spec, full_spec, full_spec, full_spec, full_spec),
                         out_specs=(row_spec, row_spec), check_vma=False)
```

```python
import functools
import math

import jax
import jax.numpy as jnp
from jax import lax
from jax.experimental import pallas as pl
from jax.experimental.pallas import tpu as pltpu
from jax.sharding import PartitionSpec as P

HEAD_DIM = 128
CHUNK = 128
SPLIT = 128
WRITES = 4
MESH = pl.DeviceIdType.MESH
F32 = jnp.float32
BF16 = jnp.bfloat16
NT = (((1,), (1,)), ((), ()))
NN = (((1,), (0,)), ((), ()))


def mm(a, b, dims=NN):
    return lax.dot_general(a, b, dims, preferred_element_type=F32)


def kernel(rows, d_model, q_heads, kv_heads,
           x_hbm, dy_hbm, wq_hbm, wk_hbm, wv_hbm, wo_hbm,
           y_v, dx_v,
           x_v, dy_v, wq_v, wk_v, wv_v, wo_v,
           qs, dot_v, k_all, v_all, kt, vt, pt, ds_t, e_buf, m_buf, l_buf, f_buf, o_v, dq_v,
           part, recv_a, recv_b, recv_c, send_c, dx_acc,
           in_sem, ag_send, ag_recv, rs_send, rs_recv):
    group = q_heads // kv_heads
    d = HEAD_DIM
    n_keys = 4 * rows
    half = group * rows
    scale = d ** -0.5
    gain = scale * math.log2(math.e)

    me = lax.axis_index("cp")
    core = lax.rem(me, 2)
    partner = me + 1 - 2 * core
    cross = lax.rem(me + 2, 4)

    barrier = pltpu.get_barrier_semaphore()
    for peer in (partner, cross):
        pl.semaphore_signal(barrier, inc=1, device_id={"cp": peer}, device_id_type=MESH)

    qcols = q_heads * d // 2
    loads = [
        pltpu.make_async_copy(wk_hbm, wk_v, in_sem.at[1]),
        pltpu.make_async_copy(x_hbm, x_v, in_sem.at[0]),
        pltpu.make_async_copy(wv_hbm, wv_v, in_sem.at[2]),
        pltpu.make_async_copy(wq_hbm.at[:, :qcols], wq_v.at[:, :qcols], in_sem.at[3]),
        pltpu.make_async_copy(wq_hbm.at[:, qcols:], wq_v.at[:, qcols:], in_sem.at[4]),
        pltpu.make_async_copy(dy_hbm, dy_v, in_sem.at[5]),
        pltpu.make_async_copy(wo_hbm.at[:qcols], wo_v.at[:qcols], in_sem.at[6]),
        pltpu.make_async_copy(wo_hbm.at[qcols:], wo_v.at[qcols:], in_sem.at[7]),
    ]
    for copy in loads:
        copy.start()

    def item(i):
        return (k_all if i % 2 == 0 else v_all).at[i // 2]

    def slot(i, s):
        return item(i).at[pl.ds(s * rows, rows)]

    def ag_copy(i, hop):
        src, dst, peer = ((0, 1, partner), (0, 2, cross), (2, 3, partner))[hop]
        return pltpu.make_async_remote_copy(
            src_ref=slot(i, src), dst_ref=slot(i, dst),
            send_sem=ag_send, recv_sem=ag_recv.at[i, hop],
            device_id={"cp": peer}, device_id_type=MESH)

    def forward(i):
        ag_copy(i, 1).wait_recv()
        ag_copy(i, 2).start()

    def transpose_item(i, ref):
        for s in range(4):
            ref[i // 2, :, s * rows:(s + 1) * rows] = slot(i, s)[...].T

    def head_of(i):
        h, j = i // group, i % group
        return h, slice(j * rows, (j + 1) * rows), slice(i * d, (i + 1) * d)

    def project_q(n):
        out = mm(x_v[...], wq_v[:, n * 2 * d:(n + 1) * 2 * d]).astype(BF16)
        for t in range(2):
            h, cols, _ = head_of(2 * n + t)
            qs[h, cols, :] = out[:, t * d:(t + 1) * d]

    def project_do(n):
        out = mm(wo_v[n * 2 * d:(n + 1) * 2 * d, :], dy_v[...], NT).astype(BF16)
        for t in range(2):
            h, cols, _ = head_of(2 * n + t)
            dot_v[h, :, cols] = out[t * d:(t + 1) * d, :]

    per_slot = rows // CHUNK

    def scores(i, s):
        h, cols, _ = head_of(i)
        j = i
        raw = mm(k_all[h, s * rows:(s + 1) * rows, :], qs[h, cols, :], NT)
        for c in range(per_slot):
            t = raw[c * CHUNK:(c + 1) * CHUNK].reshape(CHUNK // 8, 8, rows)
            m8 = jnp.max(t, axis=0) * gain
            e = jnp.exp2(t * gain - m8[None])
            e_buf[j, s * rows + c * CHUNK:s * rows + (c + 1) * CHUNK, :] = e.reshape(CHUNK, rows)
            m_buf[j, s * per_slot + c] = m8
            l_buf[j, s * per_slot + c] = jnp.sum(e, axis=0)

    def finalize(i, slots):
        h, cols, _ = head_of(i)
        j = i
        n_chunks = 4 * per_slot
        if 3 in slots:
            top = jnp.max(jnp.max(m_buf[j], axis=0), axis=0, keepdims=True)
            factor = [jnp.exp2(m_buf[j, c] - top) for c in range(n_chunks)]
            total = factor[0] * l_buf[j, 0]
            for c in range(1, n_chunks):
                total = total + factor[c] * l_buf[j, c]
            inv = 1.0 / jnp.sum(total, axis=0, keepdims=True)
            for c in range(n_chunks):
                f_buf[j, c] = factor[c] * inv
        for s in slots:
            for c in range(s * per_slot, (s + 1) * per_slot):
                e = e_buf[j, c * CHUNK:(c + 1) * CHUNK, :].reshape(CHUNK // 8, 8, rows)
                pt[h, c * CHUNK:(c + 1) * CHUNK, cols] = (e * f_buf[j, c][None]).reshape(CHUNK, rows).astype(BF16)

    def out_head(i):
        h, cols, feats = head_of(i)
        o_t = mm(vt[h], pt[h, :, cols]).astype(BF16)
        o_v[:, feats] = o_t.T
        return jnp.sum(dot_v[h, :, cols].astype(F32) * o_t.astype(F32), axis=0, keepdims=True)

    def dscore(i, delta):
        h, cols, _ = head_of(i)
        do_t = dot_v[h, :, cols]
        for s in range(4):
            keys = slice(s * rows, (s + 1) * rows)
            dp = mm(v_all[h, keys, :], do_t)
            ds_t[h, keys, cols] = (pt[h, keys, cols].astype(F32) * (dp - delta)).astype(BF16)

    def out_all(heads):
        heads = list(heads)
        delta = out_head(heads[0])
        for i, after in zip(heads, heads[1:] + [None]):
            delta_after = None if after is None else out_head(after)
            dscore(i, delta)
            delta = delta_after

    def dqs(i):
        h, cols, feats = head_of(i)
        dq_v[:, feats] = (mm(kt[h], ds_t[h, :, cols]) * scale).astype(BF16).T

    def grads(r, lo, hi):
        h = r % kv_heads
        for s in range(lo, hi):
            for t in range(rows // SPLIT):
                block = slice(s * rows + t * SPLIT, s * rows + (t + 1) * SPLIT)
                if r < kv_heads:
                    out = mm(pt[h, block, :], dot_v[h], NT)
                else:
                    out = mm(ds_t[h, block, :], qs[h])
                part[r, s, t * SPLIT:(t + 1) * SPLIT, :] = out

    def rs_copy(r, kind):
        src, dst, peer = ((part.at[r, 3], recv_a.at[r], partner),
                          (part.at[r, 1], recv_b.at[r], partner),
                          (send_c.at[r], recv_c.at[r], cross))[kind]
        return pltpu.make_async_remote_copy(
            src_ref=src, dst_ref=dst,
            send_sem=rs_send, recv_sem=rs_recv.at[r, kind],
            device_id={"cp": peer}, device_id_type=MESH)

    def reduce_cross(r):
        rs_copy(r, 0).wait_recv()
        send_c[r] = part[r, 2] + recv_a[r]
        rs_copy(r, 2).start()

    first = range(group)
    second = range(group, q_heads)
    n_pairs = q_heads // 4

    peers = [partner, cross]

    def stage(f):
        peers.reverse()
        pl.when(peers[0] != me)(f)

    def project_kv(w, kv_ref):
        out = mm(x_v[...], w[...]).astype(BF16)
        for h in range(kv_heads):
            kv_ref[h, :rows, :] = out[:, h * d:(h + 1) * d]

    def send_kv(item_of_head):
        for h in range(kv_heads):
            i = 2 * h + item_of_head
            ag_copy(i, 1).start()
            ag_copy(i, 0).start()

    @stage
    def _():
        loads[0].wait()
        loads[1].wait()
        project_kv(wk_v, k_all)

    pl.semaphore_wait(barrier, 2)
    send_kv(0)

    @stage
    def _():
        loads[2].wait()
        project_kv(wv_v, v_all)

    send_kv(1)

    @stage
    def _():
        loads[3].wait()
        for n in range(n_pairs):
            project_q(n)

    @stage
    def _():
        loads[4].wait()
        ag_copy(0, 0).wait_recv()
        for n in range(n_pairs):
            project_q(n_pairs + n)
            for i in (2 * n, 2 * n + 1):
                scores(i, 0)
                scores(i, 1)

    @stage
    def _():
        loads[5].wait()
        loads[6].wait()
        ag_copy(2, 0).wait_recv()
        for n in range(n_pairs):
            project_do(n)
            scores(group + n, 0)
            scores(group + n, 1)

    @stage
    def _():
        forward(0)
        for n in range(n_pairs):
            scores(group + n_pairs + n, 0)
            scores(group + n_pairs + n, 1)
        for n in first:
            scores(n, 2)

    def normalize_far(heads, r):
        for i in heads:
            scores(i, 3)
            if i > heads[0]:
                finalize(i - 1, (3, 2))
        finalize(heads[-1], (3, 2))
        grads(r, 3, 4)
        grads(r, 2, 3)
        rs_copy(r, 0).start()

    @stage
    def _():
        ag_copy(0, 2).wait_recv()
        normalize_far(first, 0)

    @stage
    def _():
        loads[7].wait()
        forward(1)
        forward(2)
        for n in range(n_pairs):
            project_do(n_pairs + n)
            for i in (2 * n, 2 * n + 1):
                finalize(i, (1, 0))
                scores(group + i, 2)
        grads(0, 1, 2)

    @stage
    def _():
        reduce_cross(0)
        rs_copy(0, 1).start()
        ag_copy(2, 2).wait_recv()
        normalize_far(second, 1)

    @stage
    def _():
        forward(3)
        ag_copy(1, 0).wait_recv()
        ag_copy(1, 2).wait_recv()
        transpose_item(1, vt)
        for i in second:
            finalize(i, (1, 0))
        out_all(first[:group // 2])

    @stage
    def _():
        reduce_cross(1)
        out_all(first[group // 2:])
        grads(2, 3, 4)
        grads(2, 2, 3)
        rs_copy(2, 0).start()

    @stage
    def _():
        ag_copy(3, 0).wait_recv()
        ag_copy(3, 2).wait_recv()
        transpose_item(3, vt)
        grads(0, 0, 1)
        out_all(second[:group // 2])

    @stage
    def _():
        reduce_cross(2)
        out_all(second[group // 2:])
        grads(3, 3, 4)
        grads(3, 2, 3)
        rs_copy(3, 0).start()

    @stage
    def _():
        grads(1, 0, 2)
        grads(2, 0, 2)
        rs_copy(1, 1).start()
        rs_copy(2, 1).start()

    @stage
    def _():
        reduce_cross(3)
        grads(3, 0, 2)
        transpose_item(0, kt)
        for i in first:
            dqs(i)
        transpose_item(2, kt)
        for i in second:
            dqs(i)
        rs_copy(3, 1).start()
        for n in range(d_model // 256):
            cols = slice(n * 256, (n + 1) * 256)
            y_v[:, cols] = mm(o_v[...], wo_v[:, cols]).astype(BF16)

    def own(items, factor):
        parts = []
        for r in items:
            rs_copy(r, 1).wait_recv()
            rs_copy(r, 2).wait_recv()
        for r in items:
            total = part[r, 0] + recv_b[r] + recv_c[r]
            parts.append((total * factor).astype(BF16) if factor != 1 else total.astype(BF16))
        return jnp.concatenate(parts, axis=1)

    @stage
    def _():
        dv = own((0, 1), 1)
        for n in range(d_model // 256):
            cols = slice(n * 256, (n + 1) * 256)
            dx_acc[:, cols] = mm(dq_v[...], wq_v[cols, :], NT) + mm(dv, wv_v[cols, :], NT)

    pltpu.make_async_copy(x_v, x_v, ag_send).wait()

    @stage
    def _():
        dk = own((2, 3), scale)
        for n in range(d_model // 256):
            cols = slice(n * 256, (n + 1) * 256)
            dx_v[:, cols] = (dx_acc[:, cols] + mm(dk, wk_v[cols, :], NT)).astype(BF16)

    pltpu.make_async_copy(dx_acc, dx_acc, rs_send).wait()


def write_out(y_v, dx_v, y_hbm, dx_hbm, sem):
    n = y_v.shape[0] // WRITES
    copies = []
    for i in range(WRITES):
        part = slice(i * n, (i + 1) * n)
        copies.append(pltpu.make_async_copy(dx_v.at[part], dx_hbm.at[part], sem.at[2 * i]))
        copies.append(pltpu.make_async_copy(y_v.at[part], y_hbm.at[part], sem.at[2 * i + 1]))
    for copy in copies:
        copy.start()
    for copy in copies:
        copy.wait()


def solution(mesh):
    row_spec = P(("dp", "cp"), None)
    full_spec = P(None, None)

    def local_body(x_loc, dy_loc, w_q, w_k, w_v, w_o):
        rows, d_model = x_loc.shape
        d = HEAD_DIM
        q_heads = w_q.shape[1] // d
        kv_heads = w_k.shape[1] // d
        group = q_heads // kv_heads
        n_keys = 4 * rows
        qw = q_heads * d
        hbm = pl.BlockSpec(memory_space=pltpu.HBM)
        vmem = pl.BlockSpec(memory_space=pltpu.VMEM)
        out = jax.ShapeDtypeStruct((rows, d_model), BF16)
        items = 2 * kv_heads
        y_v, dx_v = pl.pallas_call(
            functools.partial(kernel, rows, d_model, q_heads, kv_heads),
            out_shape=(out, out),
            in_specs=[hbm] * 6,
            out_specs=(vmem, vmem),
            scratch_shapes=[
                pltpu.VMEM((rows, d_model), BF16),
                pltpu.VMEM((rows, d_model), BF16),
                pltpu.VMEM((d_model, qw), BF16),
                pltpu.VMEM((d_model, kv_heads * d), BF16),
                pltpu.VMEM((d_model, kv_heads * d), BF16),
                pltpu.VMEM((qw, d_model), BF16),
                pltpu.VMEM((kv_heads, group * rows, d), BF16),
                pltpu.VMEM((kv_heads, d, group * rows), BF16),
                pltpu.VMEM((kv_heads, n_keys, d), BF16),
                pltpu.VMEM((kv_heads, n_keys, d), BF16),
                pltpu.VMEM((kv_heads, d, n_keys), BF16),
                pltpu.VMEM((kv_heads, d, n_keys), BF16),
                pltpu.VMEM((kv_heads, n_keys, group * rows), BF16),
                pltpu.VMEM((kv_heads, n_keys, group * rows), BF16),
                pltpu.VMEM((q_heads, n_keys, rows), F32),
                pltpu.VMEM((q_heads, n_keys // CHUNK, 8, rows), F32),
                pltpu.VMEM((q_heads, n_keys // CHUNK, 8, rows), F32),
                pltpu.VMEM((q_heads, n_keys // CHUNK, 8, rows), F32),
                pltpu.VMEM((rows, qw), BF16),
                pltpu.VMEM((rows, qw), BF16),
                pltpu.VMEM((items, 4, rows, d), F32),
                pltpu.VMEM((items, rows, d), F32),
                pltpu.VMEM((items, rows, d), F32),
                pltpu.VMEM((items, rows, d), F32),
                pltpu.VMEM((items, rows, d), F32),
                pltpu.VMEM((rows, d_model), F32),
                pltpu.SemaphoreType.DMA((8,)),
                pltpu.SemaphoreType.DMA,
                pltpu.SemaphoreType.DMA((items, 3)),
                pltpu.SemaphoreType.DMA,
                pltpu.SemaphoreType.DMA((items, 3)),
            ],
            compiler_params=pltpu.CompilerParams(
                collective_id=0, has_side_effects=True,
                vmem_limit_bytes=52 * 1024 * 1024),
        )(*(pltpu.with_memory_space_constraint(a, pltpu.HBM) for a in (x_loc, dy_loc, w_q, w_k, w_v, w_o)))
        return pl.pallas_call(
            write_out,
            out_shape=(out, out),
            in_specs=[pl.BlockSpec(memory_space=pl.ANY)] * 2,
            out_specs=(hbm, hbm),
            scratch_shapes=[pltpu.SemaphoreType.DMA((2 * WRITES,))],
            compiler_params=pltpu.CompilerParams(vmem_limit_bytes=4 * 1024 * 1024),
        )(y_v, dx_v)

    return jax.shard_map(local_body, mesh=mesh,
                         in_specs=(row_spec, row_spec, full_spec, full_spec, full_spec, full_spec),
                         out_specs=(row_spec, row_spec), check_vma=False)
```

```python
import functools
import math

import jax
import jax.numpy as jnp
from jax import lax
from jax.experimental import pallas as pl
from jax.experimental.pallas import tpu as pltpu
from jax.sharding import PartitionSpec as P

HEAD_DIM = 128
CHUNK = 128
SPLIT = 128
WRITES = 1
MESH = pl.DeviceIdType.MESH
F32 = jnp.float32
BF16 = jnp.bfloat16
NT = (((1,), (1,)), ((), ()))
NN = (((1,), (0,)), ((), ()))


def mm(a, b, dims=NN):
    return lax.dot_general(a, b, dims, preferred_element_type=F32)


def kernel(rows, d_model, q_heads, kv_heads,
           x_hbm, dy_hbm, wq_hbm, wk_hbm, wv_hbm, wo_hbm,
           y_v, dx_v,
           x_v, dy_v, wq_v, wk_v, wv_v, wo_v,
           qs, dot_v, k_all, v_all, kt, vt, pt, ds_t, e_buf, m_buf, l_buf, f_buf, o_v, dq_v,
           part, recv_a, recv_b, recv_c, send_c, dx_acc,
           in_sem, ag_send, ag_recv, rs_send, rs_recv):
    group = q_heads // kv_heads
    d = HEAD_DIM
    n_keys = 4 * rows
    half = group * rows
    scale = d ** -0.5
    gain = scale * math.log2(math.e)

    me = lax.axis_index("cp")
    core = lax.rem(me, 2)
    partner = me + 1 - 2 * core
    cross = lax.rem(me + 2, 4)

    barrier = pltpu.get_barrier_semaphore()
    for peer in (partner, cross):
        pl.semaphore_signal(barrier, inc=1, device_id={"cp": peer}, device_id_type=MESH)

    qcols = q_heads * d // 2
    loads = [
        pltpu.make_async_copy(wk_hbm, wk_v, in_sem.at[1]),
        pltpu.make_async_copy(x_hbm, x_v, in_sem.at[0]),
        pltpu.make_async_copy(wv_hbm, wv_v, in_sem.at[2]),
        pltpu.make_async_copy(wq_hbm.at[:, :qcols], wq_v.at[:, :qcols], in_sem.at[3]),
        pltpu.make_async_copy(wq_hbm.at[:, qcols:], wq_v.at[:, qcols:], in_sem.at[4]),
        pltpu.make_async_copy(dy_hbm, dy_v, in_sem.at[5]),
        pltpu.make_async_copy(wo_hbm.at[:qcols], wo_v.at[:qcols], in_sem.at[6]),
        pltpu.make_async_copy(wo_hbm.at[qcols:], wo_v.at[qcols:], in_sem.at[7]),
    ]
    for copy in loads:
        copy.start()

    def item(i):
        return (k_all if i % 2 == 0 else v_all).at[i // 2]

    def slot(i, s):
        return item(i).at[pl.ds(s * rows, rows)]

    def ag_copy(i, hop):
        src, dst, peer = ((0, 1, partner), (0, 2, cross), (2, 3, partner))[hop]
        return pltpu.make_async_remote_copy(
            src_ref=slot(i, src), dst_ref=slot(i, dst),
            send_sem=ag_send, recv_sem=ag_recv.at[i, hop],
            device_id={"cp": peer}, device_id_type=MESH)

    def forward(i):
        ag_copy(i, 1).wait_recv()
        ag_copy(i, 2).start()

    def transpose_item(i, ref):
        for s in range(4):
            ref[i // 2, :, s * rows:(s + 1) * rows] = slot(i, s)[...].T

    def head_of(i):
        h, j = i // group, i % group
        return h, slice(j * rows, (j + 1) * rows), slice(i * d, (i + 1) * d)

    def project_q(n):
        out = mm(x_v[...], wq_v[:, n * 2 * d:(n + 1) * 2 * d]).astype(BF16)
        for t in range(2):
            h, cols, _ = head_of(2 * n + t)
            qs[h, cols, :] = out[:, t * d:(t + 1) * d]

    def project_do(n):
        out = mm(wo_v[n * 2 * d:(n + 1) * 2 * d, :], dy_v[...], NT).astype(BF16)
        for t in range(2):
            h, cols, _ = head_of(2 * n + t)
            dot_v[h, :, cols] = out[t * d:(t + 1) * d, :]

    per_slot = rows // CHUNK

    def scores(i, s):
        h, cols, _ = head_of(i)
        j = i
        raw = mm(k_all[h, s * rows:(s + 1) * rows, :], qs[h, cols, :], NT)
        for c in range(per_slot):
            t = raw[c * CHUNK:(c + 1) * CHUNK].reshape(CHUNK // 8, 8, rows)
            m8 = jnp.max(t, axis=0) * gain
            e = jnp.exp2(t * gain - m8[None])
            e_buf[j, s * rows + c * CHUNK:s * rows + (c + 1) * CHUNK, :] = e.reshape(CHUNK, rows)
            m_buf[j, s * per_slot + c] = m8
            l_buf[j, s * per_slot + c] = jnp.sum(e, axis=0)

    def finalize(i, slots):
        h, cols, _ = head_of(i)
        j = i
        n_chunks = 4 * per_slot
        if 3 in slots:
            top = jnp.max(jnp.max(m_buf[j], axis=0), axis=0, keepdims=True)
            factor = [jnp.exp2(m_buf[j, c] - top) for c in range(n_chunks)]
            total = factor[0] * l_buf[j, 0]
            for c in range(1, n_chunks):
                total = total + factor[c] * l_buf[j, c]
            inv = 1.0 / jnp.sum(total, axis=0, keepdims=True)
            for c in range(n_chunks):
                f_buf[j, c] = factor[c] * inv
        for s in slots:
            for c in range(s * per_slot, (s + 1) * per_slot):
                e = e_buf[j, c * CHUNK:(c + 1) * CHUNK, :].reshape(CHUNK // 8, 8, rows)
                pt[h, c * CHUNK:(c + 1) * CHUNK, cols] = (e * f_buf[j, c][None]).reshape(CHUNK, rows).astype(BF16)

    def out_head(i):
        h, cols, feats = head_of(i)
        o_t = mm(vt[h], pt[h, :, cols]).astype(BF16)
        o_v[:, feats] = o_t.T
        return jnp.sum(dot_v[h, :, cols].astype(F32) * o_t.astype(F32), axis=0, keepdims=True)

    def dscore(i, delta):
        h, cols, _ = head_of(i)
        do_t = dot_v[h, :, cols]
        for s in range(4):
            keys = slice(s * rows, (s + 1) * rows)
            dp = mm(v_all[h, keys, :], do_t)
            ds_t[h, keys, cols] = (pt[h, keys, cols].astype(F32) * (dp - delta)).astype(BF16)

    def out_all(heads):
        heads = list(heads)
        delta = out_head(heads[0])
        for i, after in zip(heads, heads[1:] + [None]):
            delta_after = None if after is None else out_head(after)
            dscore(i, delta)
            delta = delta_after

    def dqs(i):
        h, cols, feats = head_of(i)
        dq_v[:, feats] = (mm(kt[h], ds_t[h, :, cols]) * scale).astype(BF16).T

    def grads(r, lo, hi):
        h = r % kv_heads
        for s in range(lo, hi):
            for t in range(rows // SPLIT):
                block = slice(s * rows + t * SPLIT, s * rows + (t + 1) * SPLIT)
                if r < kv_heads:
                    out = mm(pt[h, block, :], dot_v[h], NT)
                else:
                    out = mm(ds_t[h, block, :], qs[h])
                part[r, s, t * SPLIT:(t + 1) * SPLIT, :] = out

    def rs_copy(r, kind):
        src, dst, peer = ((part.at[r, 3], recv_a.at[r], partner),
                          (part.at[r, 1], recv_b.at[r], partner),
                          (send_c.at[r], recv_c.at[r], cross))[kind]
        return pltpu.make_async_remote_copy(
            src_ref=src, dst_ref=dst,
            send_sem=rs_send, recv_sem=rs_recv.at[r, kind],
            device_id={"cp": peer}, device_id_type=MESH)

    def reduce_cross(r):
        rs_copy(r, 0).wait_recv()
        send_c[r] = part[r, 2] + recv_a[r]
        rs_copy(r, 2).start()

    first = range(group)
    second = range(group, q_heads)
    n_pairs = q_heads // 4

    peers = [partner, cross]

    def stage(f):
        peers.reverse()
        pl.when(peers[0] != me)(f)

    def stage_at(x):
        return pl.when(me // 2 == x)

    def project_kv(w, kv_ref):
        out = mm(x_v[...], w[...]).astype(BF16)
        for h in range(kv_heads):
            kv_ref[h, :rows, :] = out[:, h * d:(h + 1) * d]

    def send_kv(item_of_head):
        for h in range(kv_heads):
            i = 2 * h + item_of_head
            ag_copy(i, 1).start()
            ag_copy(i, 0).start()

    @stage
    def _():
        loads[0].wait()
        loads[1].wait()
        project_kv(wk_v, k_all)

    pl.semaphore_wait(barrier, 2)
    send_kv(0)

    @stage
    def _():
        loads[2].wait()
        project_kv(wv_v, v_all)

    send_kv(1)

    @stage
    def _():
        loads[3].wait()
        for n in range(n_pairs):
            project_q(n)

    @stage
    def _():
        loads[4].wait()
        ag_copy(0, 0).wait_recv()
        for n in range(n_pairs):
            project_q(n_pairs + n)
            for i in (2 * n, 2 * n + 1):
                scores(i, 0)
                scores(i, 1)

    @stage_at(1)
    def _():
        forward(0)

    @stage
    def _():
        loads[5].wait()
        loads[6].wait()
        ag_copy(2, 0).wait_recv()
        for n in range(n_pairs):
            project_do(n)
            scores(group + n, 0)
            scores(group + n, 1)

    def local_rest():
        for i in second[n_pairs:]:
            scores(i, 0)
            scores(i, 1)

    @stage_at(0)
    def _():
        forward(0)
        local_rest()

    @stage
    def _():
        for n in first:
            scores(n, 2)

    def normalize_far(heads, r):
        for i in heads:
            scores(i, 3)
            if i > heads[0]:
                finalize(i - 1, (3, 2))
        finalize(heads[-1], (3, 2))
        grads(r, 3, 4)
        grads(r, 2, 3)
        rs_copy(r, 0).start()

    @stage
    def _():
        ag_copy(0, 2).wait_recv()
        normalize_far(first, 0)

    @stage
    def _():
        loads[7].wait()
        forward(2)
        for n in range(n_pairs):
            project_do(n_pairs + n)
            finalize(2 * n, (1, 0))
            finalize(2 * n + 1, (1, 0))

    @stage_at(1)
    def _():
        local_rest()

    @stage_at(1)
    def _():
        reduce_cross(0)

    @stage
    def _():
        forward(1)
        for i in second:
            scores(i, 2)
        grads(0, 1, 2)

    @stage_at(0)
    def _():
        reduce_cross(0)

    @stage
    def _():
        rs_copy(0, 1).start()
        ag_copy(2, 2).wait_recv()
        normalize_far(second, 1)

    @stage
    def _():
        forward(3)
        ag_copy(1, 0).wait_recv()
        ag_copy(1, 2).wait_recv()
        transpose_item(1, vt)
        for i in second:
            finalize(i, (1, 0))
        out_all(first[:group // 2])

    @stage
    def _():
        reduce_cross(1)
        out_all(first[group // 2:])
        grads(2, 3, 4)
        grads(2, 2, 3)
        rs_copy(2, 0).start()

    @stage
    def _():
        ag_copy(3, 0).wait_recv()
        ag_copy(3, 2).wait_recv()
        transpose_item(3, vt)
        grads(0, 0, 1)
        out_all(second[:group // 2])

    @stage
    def _():
        reduce_cross(2)
        out_all(second[group // 2:])
        grads(3, 3, 4)
        grads(3, 2, 3)
        rs_copy(3, 0).start()

    @stage
    def _():
        grads(1, 0, 2)
        grads(2, 0, 2)
        rs_copy(1, 1).start()
        rs_copy(2, 1).start()

    @stage
    def _():
        reduce_cross(3)
        grads(3, 0, 2)
        transpose_item(0, kt)
        for i in first:
            dqs(i)
        transpose_item(2, kt)
        for i in second:
            dqs(i)
        rs_copy(3, 1).start()
        for n in range(d_model // 256):
            cols = slice(n * 256, (n + 1) * 256)
            y_v[:, cols] = mm(o_v[...], wo_v[:, cols]).astype(BF16)

    def own(items, factor):
        parts = []
        for r in items:
            rs_copy(r, 1).wait_recv()
            rs_copy(r, 2).wait_recv()
        for r in items:
            total = part[r, 0] + recv_b[r] + recv_c[r]
            parts.append((total * factor).astype(BF16) if factor != 1 else total.astype(BF16))
        return jnp.concatenate(parts, axis=1)

    @stage
    def _():
        dv = own((0, 1), 1)
        for n in range(d_model // 256):
            cols = slice(n * 256, (n + 1) * 256)
            dx_acc[:, cols] = mm(dq_v[...], wq_v[cols, :], NT) + mm(dv, wv_v[cols, :], NT)

    pltpu.make_async_copy(x_v, x_v, ag_send).wait()

    @stage
    def _():
        dk = own((2, 3), scale)
        for n in range(d_model // 256):
            cols = slice(n * 256, (n + 1) * 256)
            dx_v[:, cols] = (dx_acc[:, cols] + mm(dk, wk_v[cols, :], NT)).astype(BF16)

    pltpu.make_async_copy(dx_acc, dx_acc, rs_send).wait()


def write_out(y_v, dx_v, y_hbm, dx_hbm, sem):
    n = y_v.shape[0] // WRITES
    copies = []
    for i in range(WRITES):
        part = slice(i * n, (i + 1) * n)
        copies.append(pltpu.make_async_copy(dx_v.at[part], dx_hbm.at[part], sem.at[2 * i]))
        copies.append(pltpu.make_async_copy(y_v.at[part], y_hbm.at[part], sem.at[2 * i + 1]))
    for copy in copies:
        copy.start()
    for copy in copies:
        copy.wait()


def solution(mesh):
    row_spec = P(("dp", "cp"), None)
    full_spec = P(None, None)

    def local_body(x_loc, dy_loc, w_q, w_k, w_v, w_o):
        rows, d_model = x_loc.shape
        d = HEAD_DIM
        q_heads = w_q.shape[1] // d
        kv_heads = w_k.shape[1] // d
        group = q_heads // kv_heads
        n_keys = 4 * rows
        qw = q_heads * d
        hbm = pl.BlockSpec(memory_space=pltpu.HBM)
        vmem = pl.BlockSpec(memory_space=pltpu.VMEM)
        out = jax.ShapeDtypeStruct((rows, d_model), BF16)
        items = 2 * kv_heads
        y_v, dx_v = pl.pallas_call(
            functools.partial(kernel, rows, d_model, q_heads, kv_heads),
            out_shape=(out, out),
            in_specs=[hbm] * 6,
            out_specs=(vmem, vmem),
            scratch_shapes=[
                pltpu.VMEM((rows, d_model), BF16),
                pltpu.VMEM((rows, d_model), BF16),
                pltpu.VMEM((d_model, qw), BF16),
                pltpu.VMEM((d_model, kv_heads * d), BF16),
                pltpu.VMEM((d_model, kv_heads * d), BF16),
                pltpu.VMEM((qw, d_model), BF16),
                pltpu.VMEM((kv_heads, group * rows, d), BF16),
                pltpu.VMEM((kv_heads, d, group * rows), BF16),
                pltpu.VMEM((kv_heads, n_keys, d), BF16),
                pltpu.VMEM((kv_heads, n_keys, d), BF16),
                pltpu.VMEM((kv_heads, d, n_keys), BF16),
                pltpu.VMEM((kv_heads, d, n_keys), BF16),
                pltpu.VMEM((kv_heads, n_keys, group * rows), BF16),
                pltpu.VMEM((kv_heads, n_keys, group * rows), BF16),
                pltpu.VMEM((q_heads, n_keys, rows), F32),
                pltpu.VMEM((q_heads, n_keys // CHUNK, 8, rows), F32),
                pltpu.VMEM((q_heads, n_keys // CHUNK, 8, rows), F32),
                pltpu.VMEM((q_heads, n_keys // CHUNK, 8, rows), F32),
                pltpu.VMEM((rows, qw), BF16),
                pltpu.VMEM((rows, qw), BF16),
                pltpu.VMEM((items, 4, rows, d), F32),
                pltpu.VMEM((items, rows, d), F32),
                pltpu.VMEM((items, rows, d), F32),
                pltpu.VMEM((items, rows, d), F32),
                pltpu.VMEM((items, rows, d), F32),
                pltpu.VMEM((rows, d_model), F32),
                pltpu.SemaphoreType.DMA((8,)),
                pltpu.SemaphoreType.DMA,
                pltpu.SemaphoreType.DMA((items, 3)),
                pltpu.SemaphoreType.DMA,
                pltpu.SemaphoreType.DMA((items, 3)),
            ],
            compiler_params=pltpu.CompilerParams(
                collective_id=0, has_side_effects=True,
                vmem_limit_bytes=52 * 1024 * 1024),
        )(*(pltpu.with_memory_space_constraint(a, pltpu.HBM) for a in (x_loc, dy_loc, w_q, w_k, w_v, w_o)))
        return pl.pallas_call(
            write_out,
            out_shape=(out, out),
            in_specs=[pl.BlockSpec(memory_space=pl.ANY)] * 2,
            out_specs=(hbm, hbm),
            scratch_shapes=[pltpu.SemaphoreType.DMA((2 * WRITES,))],
            compiler_params=pltpu.CompilerParams(vmem_limit_bytes=4 * 1024 * 1024),
        )(y_v, dx_v)

    return jax.shard_map(local_body, mesh=mesh,
                         in_specs=(row_spec, row_spec, full_spec, full_spec, full_spec, full_spec),
                         out_specs=(row_spec, row_spec), check_vma=False)
```

```python
import functools
import math

import jax
import jax.numpy as jnp
from jax import lax
from jax.experimental import pallas as pl
from jax.experimental.pallas import tpu as pltpu
from jax.sharding import PartitionSpec as P

HEAD_DIM = 128
CHUNK = 128
SPLIT = 128
PIECES = 3
MESH = pl.DeviceIdType.MESH
F32 = jnp.float32
BF16 = jnp.bfloat16
NT = (((1,), (1,)), ((), ()))
NN = (((1,), (0,)), ((), ()))


def mm(a, b, dims=NN):
    return lax.dot_general(a, b, dims, preferred_element_type=F32)


def kernel(rows, d_model, q_heads, kv_heads,
           x_hbm, dy_hbm, wq_hbm, wk_hbm, wv_hbm, wo_hbm,
           y_v, dx_acc, dk_v, wk_v,
           x_v, dy_v, wq_v, wv_v, wo_v,
           qs, dot_v, k_all, v_all, kt, vt, pt, ds_t, e_buf, m_buf, l_buf, f_buf, o_v, dq_v,
           part, recv_a, recv_b, recv_c, send_c,
           in_sem, ag_send, ag_recv, rs_send, rs_recv):
    group = q_heads // kv_heads
    d = HEAD_DIM
    n_keys = 4 * rows
    half = group * rows
    scale = d ** -0.5
    gain = scale * math.log2(math.e)

    me = lax.axis_index("cp")
    core = lax.rem(me, 2)
    partner = me + 1 - 2 * core
    cross = lax.rem(me + 2, 4)

    barrier = pltpu.get_barrier_semaphore()
    for peer in (partner, cross):
        pl.semaphore_signal(barrier, inc=1, device_id={"cp": peer}, device_id_type=MESH)

    qcols = q_heads * d // 2
    loads = [
        pltpu.make_async_copy(wk_hbm, wk_v, in_sem.at[1]),
        pltpu.make_async_copy(x_hbm, x_v, in_sem.at[0]),
        pltpu.make_async_copy(wv_hbm, wv_v, in_sem.at[2]),
        pltpu.make_async_copy(wq_hbm.at[:, :qcols], wq_v.at[:, :qcols], in_sem.at[3]),
        pltpu.make_async_copy(wq_hbm.at[:, qcols:], wq_v.at[:, qcols:], in_sem.at[4]),
        pltpu.make_async_copy(dy_hbm, dy_v, in_sem.at[5]),
        pltpu.make_async_copy(wo_hbm.at[:qcols], wo_v.at[:qcols], in_sem.at[6]),
        pltpu.make_async_copy(wo_hbm.at[qcols:], wo_v.at[qcols:], in_sem.at[7]),
    ]
    for copy in loads:
        copy.start()

    def item(i):
        return (k_all if i % 2 == 0 else v_all).at[i // 2]

    def slot(i, s):
        return item(i).at[pl.ds(s * rows, rows)]

    def ag_copy(i, hop):
        src, dst, peer = ((0, 1, partner), (0, 2, cross), (2, 3, partner))[hop]
        return pltpu.make_async_remote_copy(
            src_ref=slot(i, src), dst_ref=slot(i, dst),
            send_sem=ag_send, recv_sem=ag_recv.at[i, hop],
            device_id={"cp": peer}, device_id_type=MESH)

    def forward(i):
        ag_copy(i, 1).wait_recv()
        ag_copy(i, 2).start()

    def transpose_item(i, ref):
        for s in range(4):
            ref[i // 2, :, s * rows:(s + 1) * rows] = slot(i, s)[...].T

    def head_of(i):
        h, j = i // group, i % group
        return h, slice(j * rows, (j + 1) * rows), slice(i * d, (i + 1) * d)

    def project_q(n):
        out = mm(x_v[...], wq_v[:, n * 2 * d:(n + 1) * 2 * d]).astype(BF16)
        for t in range(2):
            h, cols, _ = head_of(2 * n + t)
            qs[h, cols, :] = out[:, t * d:(t + 1) * d]

    def project_do(n):
        out = mm(wo_v[n * 2 * d:(n + 1) * 2 * d, :], dy_v[...], NT).astype(BF16)
        for t in range(2):
            h, cols, _ = head_of(2 * n + t)
            dot_v[h, :, cols] = out[t * d:(t + 1) * d, :]

    per_slot = rows // CHUNK

    def scores(i, s):
        h, cols, _ = head_of(i)
        j = i
        raw = mm(k_all[h, s * rows:(s + 1) * rows, :], qs[h, cols, :], NT)
        for c in range(per_slot):
            t = raw[c * CHUNK:(c + 1) * CHUNK].reshape(CHUNK // 8, 8, rows)
            m8 = jnp.max(t, axis=0) * gain
            e = jnp.exp2(t * gain - m8[None])
            e_buf[j, s * rows + c * CHUNK:s * rows + (c + 1) * CHUNK, :] = e.reshape(CHUNK, rows)
            m_buf[j, s * per_slot + c] = m8
            l_buf[j, s * per_slot + c] = jnp.sum(e, axis=0)

    def finalize(i, slots):
        h, cols, _ = head_of(i)
        j = i
        n_chunks = 4 * per_slot
        if 3 in slots:
            top = jnp.max(jnp.max(m_buf[j], axis=0), axis=0, keepdims=True)
            factor = [jnp.exp2(m_buf[j, c] - top) for c in range(n_chunks)]
            total = factor[0] * l_buf[j, 0]
            for c in range(1, n_chunks):
                total = total + factor[c] * l_buf[j, c]
            inv = 1.0 / jnp.sum(total, axis=0, keepdims=True)
            for c in range(n_chunks):
                f_buf[j, c] = factor[c] * inv
        for s in slots:
            for c in range(s * per_slot, (s + 1) * per_slot):
                e = e_buf[j, c * CHUNK:(c + 1) * CHUNK, :].reshape(CHUNK // 8, 8, rows)
                pt[h, c * CHUNK:(c + 1) * CHUNK, cols] = (e * f_buf[j, c][None]).reshape(CHUNK, rows).astype(BF16)

    def out_head(i):
        h, cols, feats = head_of(i)
        o_t = mm(vt[h], pt[h, :, cols]).astype(BF16)
        o_v[:, feats] = o_t.T
        return jnp.sum(dot_v[h, :, cols].astype(F32) * o_t.astype(F32), axis=0, keepdims=True)

    def dscore(i, delta):
        h, cols, _ = head_of(i)
        do_t = dot_v[h, :, cols]
        for s in range(4):
            keys = slice(s * rows, (s + 1) * rows)
            dp = mm(v_all[h, keys, :], do_t)
            ds_t[h, keys, cols] = (pt[h, keys, cols].astype(F32) * (dp - delta)).astype(BF16)

    def out_all(heads):
        heads = list(heads)
        delta = out_head(heads[0])
        for i, after in zip(heads, heads[1:] + [None]):
            delta_after = None if after is None else out_head(after)
            dscore(i, delta)
            delta = delta_after

    def dqs(i):
        h, cols, feats = head_of(i)
        dq_v[:, feats] = (mm(kt[h], ds_t[h, :, cols]) * scale).astype(BF16).T

    def grads(r, lo, hi):
        h = r % kv_heads
        for s in range(lo, hi):
            for t in range(rows // SPLIT):
                block = slice(s * rows + t * SPLIT, s * rows + (t + 1) * SPLIT)
                if r < kv_heads:
                    out = mm(pt[h, block, :], dot_v[h], NT)
                else:
                    out = mm(ds_t[h, block, :], qs[h])
                part[r, s, t * SPLIT:(t + 1) * SPLIT, :] = out

    def rs_copy(r, kind):
        src, dst, peer = ((part.at[r, 3], recv_a.at[r], partner),
                          (part.at[r, 1], recv_b.at[r], partner),
                          (send_c.at[r], recv_c.at[r], cross))[kind]
        return pltpu.make_async_remote_copy(
            src_ref=src, dst_ref=dst,
            send_sem=rs_send, recv_sem=rs_recv.at[r, kind],
            device_id={"cp": peer}, device_id_type=MESH)

    def reduce_cross(r):
        rs_copy(r, 0).wait_recv()
        send_c[r] = part[r, 2] + recv_a[r]
        rs_copy(r, 2).start()

    first = range(group)
    second = range(group, q_heads)
    n_pairs = q_heads // 4

    peers = [partner, cross]

    def stage(f):
        peers.reverse()
        pl.when(peers[0] != me)(f)

    def project_kv(w, kv_ref):
        out = mm(x_v[...], w[...]).astype(BF16)
        for h in range(kv_heads):
            kv_ref[h, :rows, :] = out[:, h * d:(h + 1) * d]

    def send_kv(item_of_head):
        for h in range(kv_heads):
            i = 2 * h + item_of_head
            ag_copy(i, 1).start()
            ag_copy(i, 0).start()

    @stage
    def _():
        loads[0].wait()
        loads[1].wait()
        project_kv(wk_v, k_all)

    pl.semaphore_wait(barrier, 2)
    send_kv(0)

    @stage
    def _():
        loads[2].wait()
        project_kv(wv_v, v_all)

    send_kv(1)

    @stage
    def _():
        loads[3].wait()
        for n in range(n_pairs):
            project_q(n)

    @stage
    def _():
        loads[4].wait()
        ag_copy(0, 0).wait_recv()
        for n in range(n_pairs):
            project_q(n_pairs + n)
            for i in (2 * n, 2 * n + 1):
                scores(i, 0)
                scores(i, 1)

    @stage
    def _():
        loads[5].wait()
        loads[6].wait()
        ag_copy(2, 0).wait_recv()
        for n in range(n_pairs):
            project_do(n)
            scores(group + n, 0)
            scores(group + n, 1)

    @stage
    def _():
        forward(0)
        for n in range(n_pairs):
            scores(group + n_pairs + n, 0)
            scores(group + n_pairs + n, 1)
        for n in first:
            scores(n, 2)

    def normalize_far(heads, r):
        for i in heads:
            scores(i, 3)
            if i > heads[0]:
                finalize(i - 1, (3, 2))
        finalize(heads[-1], (3, 2))
        grads(r, 3, 4)
        grads(r, 2, 3)
        rs_copy(r, 0).start()

    @stage
    def _():
        ag_copy(0, 2).wait_recv()
        normalize_far(first, 0)

    @stage
    def _():
        loads[7].wait()
        forward(1)
        forward(2)
        for n in range(n_pairs):
            project_do(n_pairs + n)
            for i in (2 * n, 2 * n + 1):
                finalize(i, (1, 0))
                scores(group + i, 2)
        grads(0, 1, 2)

    @stage
    def _():
        reduce_cross(0)
        rs_copy(0, 1).start()
        ag_copy(2, 2).wait_recv()
        normalize_far(second, 1)

    @stage
    def _():
        forward(3)
        ag_copy(1, 0).wait_recv()
        ag_copy(1, 2).wait_recv()
        transpose_item(1, vt)
        for i in second:
            finalize(i, (1, 0))
        out_all(first[:group // 2])

    @stage
    def _():
        reduce_cross(1)
        out_all(first[group // 2:])
        grads(2, 3, 4)
        grads(2, 2, 3)
        rs_copy(2, 0).start()

    @stage
    def _():
        ag_copy(3, 0).wait_recv()
        ag_copy(3, 2).wait_recv()
        transpose_item(3, vt)
        grads(0, 0, 1)
        out_all(second[:group // 2])

    @stage
    def _():
        reduce_cross(2)
        out_all(second[group // 2:])
        grads(3, 3, 4)
        grads(3, 2, 3)
        rs_copy(3, 0).start()

    @stage
    def _():
        grads(1, 0, 2)
        grads(2, 0, 2)
        rs_copy(1, 1).start()
        rs_copy(2, 1).start()

    @stage
    def _():
        reduce_cross(3)
        grads(3, 0, 2)
        transpose_item(0, kt)
        for i in first:
            dqs(i)
        transpose_item(2, kt)
        for i in second:
            dqs(i)
        rs_copy(3, 1).start()
        for n in range(d_model // 256):
            cols = slice(n * 256, (n + 1) * 256)
            y_v[:, cols] = mm(o_v[...], wo_v[:, cols]).astype(BF16)

    def own(items, factor):
        parts = []
        for r in items:
            rs_copy(r, 1).wait_recv()
            rs_copy(r, 2).wait_recv()
        for r in items:
            total = part[r, 0] + recv_b[r] + recv_c[r]
            parts.append((total * factor).astype(BF16) if factor != 1 else total.astype(BF16))
        return jnp.concatenate(parts, axis=1)

    @stage
    def _():
        dv = own((0, 1), 1)
        for n in range(d_model // 256):
            cols = slice(n * 256, (n + 1) * 256)
            dx_acc[:, cols] = mm(dq_v[...], wq_v[cols, :], NT) + mm(dv, wv_v[cols, :], NT)

    pltpu.make_async_copy(x_v, x_v, ag_send).wait()

    @stage
    def _():
        dk_v[...] = own((2, 3), scale)

    pltpu.make_async_copy(dx_acc, dx_acc, rs_send).wait()


def finish(y_v, acc, dk, wk, y_hbm, dx_hbm, dx_v, sem):
    copies = [pltpu.make_async_copy(y_v, y_hbm, sem.at[0])]
    copies[0].start()
    width = acc.shape[1] // PIECES
    for n in range(PIECES):
        cols = slice(n * width, (n + 1) * width)
        dx_v[:, cols] = (acc[:, cols] + mm(dk[...], wk[cols, :], NT)).astype(BF16)
        copy = pltpu.make_async_copy(dx_v.at[:, cols], dx_hbm.at[:, cols], sem.at[1 + n])
        copy.start()
        copies.append(copy)
    for copy in copies:
        copy.wait()


def solution(mesh):
    row_spec = P(("dp", "cp"), None)
    full_spec = P(None, None)

    def local_body(x_loc, dy_loc, w_q, w_k, w_v, w_o):
        rows, d_model = x_loc.shape
        d = HEAD_DIM
        q_heads = w_q.shape[1] // d
        kv_heads = w_k.shape[1] // d
        group = q_heads // kv_heads
        n_keys = 4 * rows
        qw = q_heads * d
        hbm = pl.BlockSpec(memory_space=pltpu.HBM)
        vmem = pl.BlockSpec(memory_space=pltpu.VMEM)
        out = jax.ShapeDtypeStruct((rows, d_model), BF16)
        items = 2 * kv_heads
        y_v, acc, dk, wk = pl.pallas_call(
            functools.partial(kernel, rows, d_model, q_heads, kv_heads),
            out_shape=(out, jax.ShapeDtypeStruct((rows, d_model), F32),
                       jax.ShapeDtypeStruct((rows, kv_heads * d), BF16),
                       jax.ShapeDtypeStruct((d_model, kv_heads * d), BF16)),
            in_specs=[hbm] * 6,
            out_specs=(vmem,) * 4,
            scratch_shapes=[
                pltpu.VMEM((rows, d_model), BF16),
                pltpu.VMEM((rows, d_model), BF16),
                pltpu.VMEM((d_model, qw), BF16),
                pltpu.VMEM((d_model, kv_heads * d), BF16),
                pltpu.VMEM((qw, d_model), BF16),
                pltpu.VMEM((kv_heads, group * rows, d), BF16),
                pltpu.VMEM((kv_heads, d, group * rows), BF16),
                pltpu.VMEM((kv_heads, n_keys, d), BF16),
                pltpu.VMEM((kv_heads, n_keys, d), BF16),
                pltpu.VMEM((kv_heads, d, n_keys), BF16),
                pltpu.VMEM((kv_heads, d, n_keys), BF16),
                pltpu.VMEM((kv_heads, n_keys, group * rows), BF16),
                pltpu.VMEM((kv_heads, n_keys, group * rows), BF16),
                pltpu.VMEM((q_heads, n_keys, rows), F32),
                pltpu.VMEM((q_heads, n_keys // CHUNK, 8, rows), F32),
                pltpu.VMEM((q_heads, n_keys // CHUNK, 8, rows), F32),
                pltpu.VMEM((q_heads, n_keys // CHUNK, 8, rows), F32),
                pltpu.VMEM((rows, qw), BF16),
                pltpu.VMEM((rows, qw), BF16),
                pltpu.VMEM((items, 4, rows, d), F32),
                pltpu.VMEM((items, rows, d), F32),
                pltpu.VMEM((items, rows, d), F32),
                pltpu.VMEM((items, rows, d), F32),
                pltpu.VMEM((items, rows, d), F32),
                pltpu.SemaphoreType.DMA((8,)),
                pltpu.SemaphoreType.DMA,
                pltpu.SemaphoreType.DMA((items, 3)),
                pltpu.SemaphoreType.DMA,
                pltpu.SemaphoreType.DMA((items, 3)),
            ],
            compiler_params=pltpu.CompilerParams(
                collective_id=0, has_side_effects=True,
                vmem_limit_bytes=50 * 1024 * 1024),
        )(*(pltpu.with_memory_space_constraint(a, pltpu.HBM) for a in (x_loc, dy_loc, w_q, w_k, w_v, w_o)))
        return pl.pallas_call(
            finish,
            out_shape=(out, out),
            in_specs=[vmem] * 4,
            out_specs=(hbm, hbm),
            scratch_shapes=[pltpu.VMEM((rows, d_model), BF16),
                            pltpu.SemaphoreType.DMA((1 + PIECES,))],
            compiler_params=pltpu.CompilerParams(vmem_limit_bytes=8 * 1024 * 1024),
        )(y_v, acc, dk, wk)

    return jax.shard_map(local_body, mesh=mesh,
                         in_specs=(row_spec, row_spec, full_spec, full_spec, full_spec, full_spec),
                         out_specs=(row_spec, row_spec), check_vma=False)
```

```python
import functools
import math

import jax
import jax.numpy as jnp
from jax import lax
from jax.experimental import pallas as pl
from jax.experimental.pallas import tpu as pltpu
from jax.sharding import PartitionSpec as P

HEAD_DIM = 128
CHUNK = 128
SPLIT = 128
PIECES = 3
MESH = pl.DeviceIdType.MESH
F32 = jnp.float32
BF16 = jnp.bfloat16
NT = (((1,), (1,)), ((), ()))
NN = (((1,), (0,)), ((), ()))


def mm(a, b, dims=NN):
    return lax.dot_general(a, b, dims, preferred_element_type=F32)


def kernel(rows, d_model, q_heads, kv_heads,
           x_hbm, dy_hbm, wq_hbm, wk_hbm, wv_hbm, wo_hbm,
           y_v, dx_acc, dk_v, wk_v,
           x_v, dy_v, wq_v, wv_v, wo_v,
           qs, dot_v, k_all, v_all, kt, vt, pt, ds_t, e_buf, m_buf, l_buf, f_buf, o_v, dq_v,
           part, recv_a, recv_b, recv_c, send_c,
           in_sem, ag_send, far_send, ag_recv, rs_send, rs_recv):
    group = q_heads // kv_heads
    d = HEAD_DIM
    n_keys = 4 * rows
    half = group * rows
    scale = d ** -0.5
    gain = scale * math.log2(math.e)

    me = lax.axis_index("cp")
    core = lax.rem(me, 2)
    partner = me + 1 - 2 * core
    cross = lax.rem(me + 2, 4)
    far = lax.rem(partner + 2, 4)

    barrier = pltpu.get_barrier_semaphore()
    for peer in (partner, cross, far):
        pl.semaphore_signal(barrier, inc=1, device_id={"cp": peer}, device_id_type=MESH)

    qcols = q_heads * d // 2
    loads = [
        pltpu.make_async_copy(wk_hbm, wk_v, in_sem.at[1]),
        pltpu.make_async_copy(x_hbm, x_v, in_sem.at[0]),
        pltpu.make_async_copy(wv_hbm, wv_v, in_sem.at[2]),
        pltpu.make_async_copy(wq_hbm.at[:, :qcols], wq_v.at[:, :qcols], in_sem.at[3]),
        pltpu.make_async_copy(wq_hbm.at[:, qcols:], wq_v.at[:, qcols:], in_sem.at[4]),
        pltpu.make_async_copy(dy_hbm, dy_v, in_sem.at[5]),
        pltpu.make_async_copy(wo_hbm.at[:qcols], wo_v.at[:qcols], in_sem.at[6]),
        pltpu.make_async_copy(wo_hbm.at[qcols:], wo_v.at[qcols:], in_sem.at[7]),
    ]
    for copy in loads:
        copy.start()

    def item(i):
        return (k_all if i % 2 == 0 else v_all).at[i // 2]

    def slot(i, s):
        return item(i).at[pl.ds(s * rows, rows)]

    def ag_copy(i, hop):
        src, dst, peer = ((0, 1, partner), (0, 2, cross), (2, 3, partner))[hop]
        return pltpu.make_async_remote_copy(
            src_ref=slot(i, src), dst_ref=slot(i, dst),
            send_sem=ag_send, recv_sem=ag_recv.at[i, hop],
            device_id={"cp": peer}, device_id_type=MESH)

    def first_copy(src, peer):
        return pltpu.make_async_remote_copy(
            src_ref=slot(0, src), dst_ref=slot(0, 3),
            send_sem=far_send, recv_sem=ag_recv.at[0, 2],
            device_id={"cp": peer}, device_id_type=MESH)

    def forward(i):
        ag_copy(i, 1).wait_recv()
        if i > 0:
            ag_copy(i, 2).start()
            return

        @pl.when(me < 2)
        def _():
            first_copy(2, partner).start()

    def transpose_item(i, ref):
        for s in range(4):
            ref[i // 2, :, s * rows:(s + 1) * rows] = slot(i, s)[...].T

    def head_of(i):
        h, j = i // group, i % group
        return h, slice(j * rows, (j + 1) * rows), slice(i * d, (i + 1) * d)

    def project_q(n):
        out = mm(x_v[...], wq_v[:, n * 2 * d:(n + 1) * 2 * d]).astype(BF16)
        for t in range(2):
            h, cols, _ = head_of(2 * n + t)
            qs[h, cols, :] = out[:, t * d:(t + 1) * d]

    def project_do(n):
        out = mm(wo_v[n * 2 * d:(n + 1) * 2 * d, :], dy_v[...], NT).astype(BF16)
        for t in range(2):
            h, cols, _ = head_of(2 * n + t)
            dot_v[h, :, cols] = out[t * d:(t + 1) * d, :]

    per_slot = rows // CHUNK

    def scores(i, s):
        h, cols, _ = head_of(i)
        j = i
        raw = mm(k_all[h, s * rows:(s + 1) * rows, :], qs[h, cols, :], NT)
        for c in range(per_slot):
            t = raw[c * CHUNK:(c + 1) * CHUNK].reshape(CHUNK // 8, 8, rows)
            m8 = jnp.max(t, axis=0) * gain
            e = jnp.exp2(t * gain - m8[None])
            e_buf[j, s * rows + c * CHUNK:s * rows + (c + 1) * CHUNK, :] = e.reshape(CHUNK, rows)
            m_buf[j, s * per_slot + c] = m8
            l_buf[j, s * per_slot + c] = jnp.sum(e, axis=0)

    def finalize(i, slots):
        h, cols, _ = head_of(i)
        j = i
        n_chunks = 4 * per_slot
        if 3 in slots:
            top = jnp.max(jnp.max(m_buf[j], axis=0), axis=0, keepdims=True)
            factor = [jnp.exp2(m_buf[j, c] - top) for c in range(n_chunks)]
            total = factor[0] * l_buf[j, 0]
            for c in range(1, n_chunks):
                total = total + factor[c] * l_buf[j, c]
            inv = 1.0 / jnp.sum(total, axis=0, keepdims=True)
            for c in range(n_chunks):
                f_buf[j, c] = factor[c] * inv
        for s in slots:
            for c in range(s * per_slot, (s + 1) * per_slot):
                e = e_buf[j, c * CHUNK:(c + 1) * CHUNK, :].reshape(CHUNK // 8, 8, rows)
                pt[h, c * CHUNK:(c + 1) * CHUNK, cols] = (e * f_buf[j, c][None]).reshape(CHUNK, rows).astype(BF16)

    def out_head(i):
        h, cols, feats = head_of(i)
        o_t = mm(vt[h], pt[h, :, cols]).astype(BF16)
        o_v[:, feats] = o_t.T
        return jnp.sum(dot_v[h, :, cols].astype(F32) * o_t.astype(F32), axis=0, keepdims=True)

    def dscore(i, delta):
        h, cols, _ = head_of(i)
        do_t = dot_v[h, :, cols]
        for s in range(4):
            keys = slice(s * rows, (s + 1) * rows)
            dp = mm(v_all[h, keys, :], do_t)
            ds_t[h, keys, cols] = (pt[h, keys, cols].astype(F32) * (dp - delta)).astype(BF16)

    def out_all(heads):
        heads = list(heads)
        delta = out_head(heads[0])
        for i, after in zip(heads, heads[1:] + [None]):
            delta_after = None if after is None else out_head(after)
            dscore(i, delta)
            delta = delta_after

    def dqs(i):
        h, cols, feats = head_of(i)
        dq_v[:, feats] = (mm(kt[h], ds_t[h, :, cols]) * scale).astype(BF16).T

    def grads(r, lo, hi):
        h = r % kv_heads
        for s in range(lo, hi):
            for t in range(rows // SPLIT):
                block = slice(s * rows + t * SPLIT, s * rows + (t + 1) * SPLIT)
                if r < kv_heads:
                    out = mm(pt[h, block, :], dot_v[h], NT)
                else:
                    out = mm(ds_t[h, block, :], qs[h])
                part[r, s, t * SPLIT:(t + 1) * SPLIT, :] = out

    def rs_copy(r, kind):
        src, dst, peer = ((part.at[r, 3], recv_a.at[r], partner),
                          (part.at[r, 1], recv_b.at[r], partner),
                          (send_c.at[r], recv_c.at[r], cross))[kind]
        return pltpu.make_async_remote_copy(
            src_ref=src, dst_ref=dst,
            send_sem=rs_send, recv_sem=rs_recv.at[r, kind],
            device_id={"cp": peer}, device_id_type=MESH)

    def reduce_cross(r):
        rs_copy(r, 0).wait_recv()
        send_c[r] = part[r, 2] + recv_a[r]
        rs_copy(r, 2).start()

    first = range(group)
    second = range(group, q_heads)
    n_pairs = q_heads // 4

    peers = [partner, cross]

    def stage(f):
        peers.reverse()
        pl.when(peers[0] != me)(f)

    def project_kv(w, kv_ref):
        out = mm(x_v[...], w[...]).astype(BF16)
        for h in range(kv_heads):
            kv_ref[h, :rows, :] = out[:, h * d:(h + 1) * d]

    def send_kv(item_of_head):
        for h in range(kv_heads):
            i = 2 * h + item_of_head
            ag_copy(i, 1).start()
            if i == 0:
                @pl.when(me < 2)
                def _():
                    first_copy(0, far).start()
            ag_copy(i, 0).start()

    @stage
    def _():
        loads[0].wait()
        loads[1].wait()
        project_kv(wk_v, k_all)

    pl.semaphore_wait(barrier, 3)
    send_kv(0)

    @stage
    def _():
        loads[2].wait()
        project_kv(wv_v, v_all)

    send_kv(1)

    @stage
    def _():
        loads[3].wait()
        for n in range(n_pairs):
            project_q(n)

    @stage
    def _():
        loads[4].wait()
        ag_copy(0, 0).wait_recv()
        for n in range(n_pairs):
            project_q(n_pairs + n)
            for i in (2 * n, 2 * n + 1):
                scores(i, 0)
                scores(i, 1)

    @stage
    def _():
        loads[5].wait()
        loads[6].wait()
        ag_copy(2, 0).wait_recv()
        for n in range(n_pairs):
            project_do(n)
            scores(group + n, 0)
            scores(group + n, 1)

    @stage
    def _():
        forward(0)
        for n in range(n_pairs):
            scores(group + n_pairs + n, 0)
            scores(group + n_pairs + n, 1)
        for n in first:
            scores(n, 2)

    def normalize_far(heads, r):
        for i in heads:
            scores(i, 3)
            if i > heads[0]:
                finalize(i - 1, (3, 2))
        finalize(heads[-1], (3, 2))
        grads(r, 3, 4)
        grads(r, 2, 3)
        rs_copy(r, 0).start()

    @stage
    def _():
        ag_copy(0, 2).wait_recv()
        normalize_far(first, 0)

    @stage
    def _():
        loads[7].wait()
        forward(1)
        forward(2)
        for n in range(n_pairs):
            project_do(n_pairs + n)
            for i in (2 * n, 2 * n + 1):
                finalize(i, (1, 0))
                scores(group + i, 2)
        grads(0, 1, 2)

    @stage
    def _():
        reduce_cross(0)
        rs_copy(0, 1).start()
        ag_copy(2, 2).wait_recv()
        normalize_far(second, 1)

    @stage
    def _():
        forward(3)
        ag_copy(1, 0).wait_recv()
        ag_copy(1, 2).wait_recv()
        transpose_item(1, vt)
        for i in second:
            finalize(i, (1, 0))
        out_all(first[:group // 2])

    @stage
    def _():
        reduce_cross(1)
        out_all(first[group // 2:])
        grads(2, 3, 4)
        grads(2, 2, 3)
        rs_copy(2, 0).start()

    @stage
    def _():
        ag_copy(3, 0).wait_recv()
        ag_copy(3, 2).wait_recv()
        transpose_item(3, vt)
        grads(0, 0, 1)
        out_all(second[:group // 2])

    @stage
    def _():
        reduce_cross(2)
        out_all(second[group // 2:])
        grads(3, 3, 4)
        grads(3, 2, 3)
        rs_copy(3, 0).start()

    @stage
    def _():
        grads(1, 0, 2)
        grads(2, 0, 2)
        rs_copy(1, 1).start()
        rs_copy(2, 1).start()

    @stage
    def _():
        reduce_cross(3)
        grads(3, 0, 2)
        transpose_item(0, kt)
        for i in first:
            dqs(i)
        transpose_item(2, kt)
        for i in second:
            dqs(i)
        rs_copy(3, 1).start()
        for n in range(d_model // 256):
            cols = slice(n * 256, (n + 1) * 256)
            y_v[:, cols] = mm(o_v[...], wo_v[:, cols]).astype(BF16)

    def own(items, factor):
        parts = []
        for r in items:
            rs_copy(r, 1).wait_recv()
            rs_copy(r, 2).wait_recv()
        for r in items:
            total = part[r, 0] + recv_b[r] + recv_c[r]
            parts.append((total * factor).astype(BF16) if factor != 1 else total.astype(BF16))
        return jnp.concatenate(parts, axis=1)

    @stage
    def _():
        dv = own((0, 1), 1)
        for n in range(d_model // 256):
            cols = slice(n * 256, (n + 1) * 256)
            dx_acc[:, cols] = mm(dq_v[...], wq_v[cols, :], NT) + mm(dv, wv_v[cols, :], NT)

    sent = wv_v.at[pl.ds(0, (6 * kv_heads - 1) * rows * d // wv_v.shape[1])]
    pltpu.make_async_copy(sent, sent, ag_send).wait()

    @pl.when(me < 2)
    def _():
        both = k_all.at[0, pl.ds(0, 2 * rows)]
        pltpu.make_async_copy(both, both, far_send).wait()

    @stage
    def _():
        dk_v[...] = own((2, 3), scale)

    pltpu.make_async_copy(dx_acc, dx_acc, rs_send).wait()


def finish(y_v, acc, dk, wk, y_hbm, dx_hbm, dx_v, sem):
    copies = [pltpu.make_async_copy(y_v, y_hbm, sem.at[0])]
    copies[0].start()
    width = acc.shape[1] // PIECES
    for n in range(PIECES):
        cols = slice(n * width, (n + 1) * width)
        dx_v[:, cols] = (acc[:, cols] + mm(dk[...], wk[cols, :], NT)).astype(BF16)
        copy = pltpu.make_async_copy(dx_v.at[:, cols], dx_hbm.at[:, cols], sem.at[1 + n])
        copy.start()
        copies.append(copy)
    for copy in copies:
        copy.wait()


def solution(mesh):
    row_spec = P(("dp", "cp"), None)
    full_spec = P(None, None)

    def local_body(x_loc, dy_loc, w_q, w_k, w_v, w_o):
        rows, d_model = x_loc.shape
        d = HEAD_DIM
        q_heads = w_q.shape[1] // d
        kv_heads = w_k.shape[1] // d
        group = q_heads // kv_heads
        n_keys = 4 * rows
        qw = q_heads * d
        hbm = pl.BlockSpec(memory_space=pltpu.HBM)
        vmem = pl.BlockSpec(memory_space=pltpu.VMEM)
        out = jax.ShapeDtypeStruct((rows, d_model), BF16)
        items = 2 * kv_heads
        y_v, acc, dk, wk = pl.pallas_call(
            functools.partial(kernel, rows, d_model, q_heads, kv_heads),
            out_shape=(out, jax.ShapeDtypeStruct((rows, d_model), F32),
                       jax.ShapeDtypeStruct((rows, kv_heads * d), BF16),
                       jax.ShapeDtypeStruct((d_model, kv_heads * d), BF16)),
            in_specs=[hbm] * 6,
            out_specs=(vmem,) * 4,
            scratch_shapes=[
                pltpu.VMEM((rows, d_model), BF16),
                pltpu.VMEM((rows, d_model), BF16),
                pltpu.VMEM((d_model, qw), BF16),
                pltpu.VMEM((d_model, kv_heads * d), BF16),
                pltpu.VMEM((qw, d_model), BF16),
                pltpu.VMEM((kv_heads, group * rows, d), BF16),
                pltpu.VMEM((kv_heads, d, group * rows), BF16),
                pltpu.VMEM((kv_heads, n_keys, d), BF16),
                pltpu.VMEM((kv_heads, n_keys, d), BF16),
                pltpu.VMEM((kv_heads, d, n_keys), BF16),
                pltpu.VMEM((kv_heads, d, n_keys), BF16),
                pltpu.VMEM((kv_heads, n_keys, group * rows), BF16),
                pltpu.VMEM((kv_heads, n_keys, group * rows), BF16),
                pltpu.VMEM((q_heads, n_keys, rows), F32),
                pltpu.VMEM((q_heads, n_keys // CHUNK, 8, rows), F32),
                pltpu.VMEM((q_heads, n_keys // CHUNK, 8, rows), F32),
                pltpu.VMEM((q_heads, n_keys // CHUNK, 8, rows), F32),
                pltpu.VMEM((rows, qw), BF16),
                pltpu.VMEM((rows, qw), BF16),
                pltpu.VMEM((items, 4, rows, d), F32),
                pltpu.VMEM((items, rows, d), F32),
                pltpu.VMEM((items, rows, d), F32),
                pltpu.VMEM((items, rows, d), F32),
                pltpu.VMEM((items, rows, d), F32),
                pltpu.SemaphoreType.DMA((8,)),
                pltpu.SemaphoreType.DMA,
                pltpu.SemaphoreType.DMA,
                pltpu.SemaphoreType.DMA((items, 3)),
                pltpu.SemaphoreType.DMA,
                pltpu.SemaphoreType.DMA((items, 3)),
            ],
            compiler_params=pltpu.CompilerParams(
                collective_id=0, has_side_effects=True,
                vmem_limit_bytes=50 * 1024 * 1024),
        )(*(pltpu.with_memory_space_constraint(a, pltpu.HBM) for a in (x_loc, dy_loc, w_q, w_k, w_v, w_o)))
        return pl.pallas_call(
            finish,
            out_shape=(out, out),
            in_specs=[vmem] * 4,
            out_specs=(hbm, hbm),
            scratch_shapes=[pltpu.VMEM((rows, d_model), BF16),
                            pltpu.SemaphoreType.DMA((1 + PIECES,))],
            compiler_params=pltpu.CompilerParams(vmem_limit_bytes=8 * 1024 * 1024),
        )(y_v, acc, dk, wk)

    return jax.shard_map(local_body, mesh=mesh,
                         in_specs=(row_spec, row_spec, full_spec, full_spec, full_spec, full_spec),
                         out_specs=(row_spec, row_spec), check_vma=False)
```

```python
import functools
import math

import jax
import jax.numpy as jnp
from jax import lax
from jax.experimental import pallas as pl
from jax.experimental.pallas import tpu as pltpu
from jax.sharding import PartitionSpec as P

HEAD_DIM = 128
CHUNK = 128
SPLIT = 128
PIECES = 3
MESH = pl.DeviceIdType.MESH
F32 = jnp.float32
BF16 = jnp.bfloat16
NT = (((1,), (1,)), ((), ()))
NN = (((1,), (0,)), ((), ()))


def mm(a, b, dims=NN):
    return lax.dot_general(a, b, dims, preferred_element_type=F32)


def kernel(rows, d_model, q_heads, kv_heads,
           x_hbm, dy_hbm, wq_hbm, wk_hbm, wv_hbm, wo_hbm,
           y_v, dx_acc, dk_v, wk_v,
           x_v, dy_v, wq_v, wv_v, wo_v,
           qs, dot_v, k_all, v_all, kt, vt, pt, ds_t, e_buf, m_buf, l_buf, f_buf, o_v, dq_v,
           part, recv_a, recv_b, recv_c, send_c,
           in_sem, ag_send, ag_recv, rs_send, rs_recv):
    group = q_heads // kv_heads
    d = HEAD_DIM
    n_keys = 4 * rows
    half = group * rows
    scale = d ** -0.5
    gain = scale * math.log2(math.e)

    me = lax.axis_index("cp")
    core = lax.rem(me, 2)
    partner = me + 1 - 2 * core
    cross = lax.rem(me + 2, 4)

    barrier = pltpu.get_barrier_semaphore()
    for peer in (partner, cross):
        pl.semaphore_signal(barrier, inc=1, device_id={"cp": peer}, device_id_type=MESH)

    qcols = q_heads * d // 2
    loads = [
        pltpu.make_async_copy(wk_hbm, wk_v, in_sem.at[1]),
        pltpu.make_async_copy(x_hbm, x_v, in_sem.at[0]),
        pltpu.make_async_copy(wv_hbm, wv_v, in_sem.at[2]),
        pltpu.make_async_copy(wq_hbm.at[:, :qcols], wq_v.at[:, :qcols], in_sem.at[3]),
        pltpu.make_async_copy(wq_hbm.at[:, qcols:], wq_v.at[:, qcols:], in_sem.at[4]),
        pltpu.make_async_copy(dy_hbm, dy_v, in_sem.at[5]),
        pltpu.make_async_copy(wo_hbm.at[:qcols], wo_v.at[:qcols], in_sem.at[6]),
        pltpu.make_async_copy(wo_hbm.at[qcols:], wo_v.at[qcols:], in_sem.at[7]),
    ]
    for copy in loads:
        copy.start()

    def item(i):
        return (k_all if i % 2 == 0 else v_all).at[i // 2]

    def slot(i, s):
        return item(i).at[pl.ds(s * rows, rows)]

    def ag_copy(i, hop):
        src, dst, peer = ((0, 1, partner), (0, 2, cross), (2, 3, partner))[hop]
        return pltpu.make_async_remote_copy(
            src_ref=slot(i, src), dst_ref=slot(i, dst),
            send_sem=ag_send, recv_sem=ag_recv.at[i, hop],
            device_id={"cp": peer}, device_id_type=MESH)

    def forward(i):
        ag_copy(i, 1).wait_recv()
        ag_copy(i, 2).start()

    def transpose_item(i, ref):
        for s in range(4):
            ref[i // 2, :, s * rows:(s + 1) * rows] = slot(i, s)[...].T

    def head_of(i):
        h, j = i // group, i % group
        return h, slice(j * rows, (j + 1) * rows), slice(i * d, (i + 1) * d)

    def project_q(n):
        out = mm(x_v[...], wq_v[:, n * 2 * d:(n + 1) * 2 * d]).astype(BF16)
        for t in range(2):
            h, cols, _ = head_of(2 * n + t)
            qs[h, cols, :] = out[:, t * d:(t + 1) * d]

    def project_do(n):
        out = mm(wo_v[n * 2 * d:(n + 1) * 2 * d, :], dy_v[...], NT).astype(BF16)
        for t in range(2):
            h, cols, _ = head_of(2 * n + t)
            dot_v[h, :, cols] = out[t * d:(t + 1) * d, :]

    per_slot = rows // CHUNK

    def scores(i, s):
        h, cols, _ = head_of(i)
        j = i
        raw = mm(k_all[h, s * rows:(s + 1) * rows, :], qs[h, cols, :], NT)
        for c in range(per_slot):
            t = raw[c * CHUNK:(c + 1) * CHUNK].reshape(CHUNK // 8, 8, rows)
            m8 = jnp.max(t, axis=0) * gain
            e = jnp.exp2(t * gain - m8[None])
            e_buf[j, s * rows + c * CHUNK:s * rows + (c + 1) * CHUNK, :] = e.reshape(CHUNK, rows)
            m_buf[j, s * per_slot + c] = m8
            l_buf[j, s * per_slot + c] = jnp.sum(e, axis=0)

    def finalize(i, slots):
        h, cols, _ = head_of(i)
        j = i
        n_chunks = 4 * per_slot
        if 3 in slots:
            top = jnp.max(jnp.max(m_buf[j], axis=0), axis=0, keepdims=True)
            factor = [jnp.exp2(m_buf[j, c] - top) for c in range(n_chunks)]
            total = factor[0] * l_buf[j, 0]
            for c in range(1, n_chunks):
                total = total + factor[c] * l_buf[j, c]
            inv = 1.0 / jnp.sum(total, axis=0, keepdims=True)
            for c in range(n_chunks):
                f_buf[j, c] = factor[c] * inv
        for s in slots:
            for c in range(s * per_slot, (s + 1) * per_slot):
                e = e_buf[j, c * CHUNK:(c + 1) * CHUNK, :].reshape(CHUNK // 8, 8, rows)
                pt[h, c * CHUNK:(c + 1) * CHUNK, cols] = (e * f_buf[j, c][None]).reshape(CHUNK, rows).astype(BF16)

    def out_head(i):
        h, cols, feats = head_of(i)
        o_t = mm(vt[h], pt[h, :, cols]).astype(BF16)
        o_v[:, feats] = o_t.T
        return jnp.sum(dot_v[h, :, cols].astype(F32) * o_t.astype(F32), axis=0, keepdims=True)

    def dscore(i, delta):
        h, cols, _ = head_of(i)
        do_t = dot_v[h, :, cols]
        for s in range(4):
            keys = slice(s * rows, (s + 1) * rows)
            dp = mm(v_all[h, keys, :], do_t)
            ds_t[h, keys, cols] = (pt[h, keys, cols].astype(F32) * (dp - delta)).astype(BF16)

    def out_all(heads):
        heads = list(heads)
        delta = out_head(heads[0])
        for i, after in zip(heads, heads[1:] + [None]):
            delta_after = None if after is None else out_head(after)
            dscore(i, delta)
            delta = delta_after

    def dqs(i):
        h, cols, feats = head_of(i)
        dq_v[:, feats] = (mm(kt[h], ds_t[h, :, cols]) * scale).astype(BF16).T

    def grads(r, lo, hi):
        h = r % kv_heads
        for s in range(lo, hi):
            for t in range(rows // SPLIT):
                block = slice(s * rows + t * SPLIT, s * rows + (t + 1) * SPLIT)
                if r < kv_heads:
                    out = mm(pt[h, block, :], dot_v[h], NT)
                else:
                    out = mm(ds_t[h, block, :], qs[h])
                part[r, s, t * SPLIT:(t + 1) * SPLIT, :] = out

    def rs_copy(r, kind):
        src, dst, peer = ((part.at[r, 3], recv_a.at[r], partner),
                          (part.at[r, 1], recv_b.at[r], partner),
                          (send_c.at[r], recv_c.at[r], cross))[kind]
        return pltpu.make_async_remote_copy(
            src_ref=src, dst_ref=dst,
            send_sem=rs_send, recv_sem=rs_recv.at[r, kind],
            device_id={"cp": peer}, device_id_type=MESH)

    def reduce_cross(r):
        rs_copy(r, 0).wait_recv()
        send_c[r] = part[r, 2] + recv_a[r]
        rs_copy(r, 2).start()

    first = range(group)
    second = range(group, q_heads)
    n_pairs = q_heads // 4

    peers = [partner, cross]

    def stage(f):
        peers.reverse()
        pl.when(peers[0] != me)(f)

    def project_kv(w, kv_ref):
        out = mm(x_v[...], w[...]).astype(BF16)
        for h in range(kv_heads):
            kv_ref[h, :rows, :] = out[:, h * d:(h + 1) * d]

    def send_kv(item_of_head):
        for h in range(kv_heads):
            i = 2 * h + item_of_head
            ag_copy(i, 1).start()
            ag_copy(i, 0).start()

    @stage
    def _():
        loads[0].wait()
        loads[1].wait()
        project_kv(wk_v, k_all)

    pl.semaphore_wait(barrier, 2)
    send_kv(0)

    @stage
    def _():
        loads[2].wait()
        project_kv(wv_v, v_all)

    send_kv(1)

    @stage
    def _():
        loads[3].wait()
        for n in range(n_pairs):
            project_q(n)

    @stage
    def _():
        loads[4].wait()
        ag_copy(0, 0).wait_recv()
        for n in range(n_pairs):
            project_q(n_pairs + n)
            for i in (2 * n, 2 * n + 1):
                scores(i, 0)
                scores(i, 1)

    @stage
    def _():
        loads[5].wait()
        loads[6].wait()
        ag_copy(2, 0).wait_recv()
        for n in range(n_pairs):
            project_do(n)
            scores(group + n, 0)
            scores(group + n, 1)

    @stage
    def _():
        forward(0)
        for n in range(n_pairs):
            scores(group + n_pairs + n, 0)
            scores(group + n_pairs + n, 1)
        for n in first:
            scores(n, 2)

    def normalize_far(heads, r, filler=None):
        if filler is not None:
            for n in range(n_pairs):
                filler(n)
        for k, i in enumerate(heads):
            scores(i, 3)
            if k > 0:
                finalize(i - 1, (3, 2))
        finalize(heads[-1], (3, 2))
        grads(r, 3, 4)
        grads(r, 2, 3)
        rs_copy(r, 0).start()

    @stage
    def _():
        ag_copy(0, 2).wait_recv()
        normalize_far(first, 0)

    @stage
    def _():
        forward(2)
        for n in first:
            finalize(n, (1, 0))
            scores(group + n, 2)
        grads(0, 1, 2)

    @stage
    def _():
        reduce_cross(0)
        rs_copy(0, 1).start()
        forward(1)
        loads[7].wait()
        ag_copy(2, 2).wait_recv()
        normalize_far(second, 1, lambda n: project_do(n_pairs + n))

    @stage
    def _():
        forward(3)
        ag_copy(1, 0).wait_recv()
        ag_copy(1, 2).wait_recv()
        transpose_item(1, vt)
        for i in second:
            finalize(i, (1, 0))
        out_all(first[:group // 2])

    @stage
    def _():
        reduce_cross(1)
        out_all(first[group // 2:])
        grads(2, 3, 4)
        grads(2, 2, 3)
        rs_copy(2, 0).start()

    @stage
    def _():
        ag_copy(3, 0).wait_recv()
        ag_copy(3, 2).wait_recv()
        transpose_item(3, vt)
        grads(0, 0, 1)
        out_all(second[:group // 2])

    @stage
    def _():
        reduce_cross(2)
        out_all(second[group // 2:])
        grads(3, 3, 4)
        grads(3, 2, 3)
        rs_copy(3, 0).start()

    @stage
    def _():
        grads(1, 0, 2)
        grads(2, 0, 2)
        rs_copy(1, 1).start()
        rs_copy(2, 1).start()

    @stage
    def _():
        reduce_cross(3)
        grads(3, 0, 2)
        transpose_item(0, kt)
        for i in first:
            dqs(i)
        transpose_item(2, kt)
        for i in second:
            dqs(i)
        rs_copy(3, 1).start()
        for n in range(d_model // 256):
            cols = slice(n * 256, (n + 1) * 256)
            y_v[:, cols] = mm(o_v[...], wo_v[:, cols]).astype(BF16)

    def own(items, factor):
        parts = []
        for r in items:
            rs_copy(r, 1).wait_recv()
            rs_copy(r, 2).wait_recv()
        for r in items:
            total = part[r, 0] + recv_b[r] + recv_c[r]
            parts.append((total * factor).astype(BF16) if factor != 1 else total.astype(BF16))
        return jnp.concatenate(parts, axis=1)

    @stage
    def _():
        dv = own((0, 1), 1)
        for n in range(d_model // 256):
            cols = slice(n * 256, (n + 1) * 256)
            dx_acc[:, cols] = mm(dq_v[...], wq_v[cols, :], NT) + mm(dv, wv_v[cols, :], NT)

    pltpu.make_async_copy(x_v, x_v, ag_send).wait()

    @stage
    def _():
        dk_v[...] = own((2, 3), scale)

    pltpu.make_async_copy(dx_acc, dx_acc, rs_send).wait()


def finish(y_v, acc, dk, wk, y_hbm, dx_hbm, dx_v, sem):
    copies = [pltpu.make_async_copy(y_v, y_hbm, sem.at[0])]
    copies[0].start()
    width = acc.shape[1] // PIECES
    for n in range(PIECES):
        cols = slice(n * width, (n + 1) * width)
        dx_v[:, cols] = (acc[:, cols] + mm(dk[...], wk[cols, :], NT)).astype(BF16)
        copy = pltpu.make_async_copy(dx_v.at[:, cols], dx_hbm.at[:, cols], sem.at[1 + n])
        copy.start()
        copies.append(copy)
    for copy in copies:
        copy.wait()


def solution(mesh):
    row_spec = P(("dp", "cp"), None)
    full_spec = P(None, None)

    def local_body(x_loc, dy_loc, w_q, w_k, w_v, w_o):
        rows, d_model = x_loc.shape
        d = HEAD_DIM
        q_heads = w_q.shape[1] // d
        kv_heads = w_k.shape[1] // d
        group = q_heads // kv_heads
        n_keys = 4 * rows
        qw = q_heads * d
        hbm = pl.BlockSpec(memory_space=pltpu.HBM)
        vmem = pl.BlockSpec(memory_space=pltpu.VMEM)
        out = jax.ShapeDtypeStruct((rows, d_model), BF16)
        items = 2 * kv_heads
        y_v, acc, dk, wk = pl.pallas_call(
            functools.partial(kernel, rows, d_model, q_heads, kv_heads),
            out_shape=(out, jax.ShapeDtypeStruct((rows, d_model), F32),
                       jax.ShapeDtypeStruct((rows, kv_heads * d), BF16),
                       jax.ShapeDtypeStruct((d_model, kv_heads * d), BF16)),
            in_specs=[hbm] * 6,
            out_specs=(vmem,) * 4,
            scratch_shapes=[
                pltpu.VMEM((rows, d_model), BF16),
                pltpu.VMEM((rows, d_model), BF16),
                pltpu.VMEM((d_model, qw), BF16),
                pltpu.VMEM((d_model, kv_heads * d), BF16),
                pltpu.VMEM((qw, d_model), BF16),
                pltpu.VMEM((kv_heads, group * rows, d), BF16),
                pltpu.VMEM((kv_heads, d, group * rows), BF16),
                pltpu.VMEM((kv_heads, n_keys, d), BF16),
                pltpu.VMEM((kv_heads, n_keys, d), BF16),
                pltpu.VMEM((kv_heads, d, n_keys), BF16),
                pltpu.VMEM((kv_heads, d, n_keys), BF16),
                pltpu.VMEM((kv_heads, n_keys, group * rows), BF16),
                pltpu.VMEM((kv_heads, n_keys, group * rows), BF16),
                pltpu.VMEM((q_heads, n_keys, rows), F32),
                pltpu.VMEM((q_heads, n_keys // CHUNK, 8, rows), F32),
                pltpu.VMEM((q_heads, n_keys // CHUNK, 8, rows), F32),
                pltpu.VMEM((q_heads, n_keys // CHUNK, 8, rows), F32),
                pltpu.VMEM((rows, qw), BF16),
                pltpu.VMEM((rows, qw), BF16),
                pltpu.VMEM((items, 4, rows, d), F32),
                pltpu.VMEM((items, rows, d), F32),
                pltpu.VMEM((items, rows, d), F32),
                pltpu.VMEM((items, rows, d), F32),
                pltpu.VMEM((items, rows, d), F32),
                pltpu.SemaphoreType.DMA((8,)),
                pltpu.SemaphoreType.DMA,
                pltpu.SemaphoreType.DMA((items, 3)),
                pltpu.SemaphoreType.DMA,
                pltpu.SemaphoreType.DMA((items, 3)),
            ],
            compiler_params=pltpu.CompilerParams(
                collective_id=0, has_side_effects=True,
                vmem_limit_bytes=50 * 1024 * 1024),
        )(*(pltpu.with_memory_space_constraint(a, pltpu.HBM) for a in (x_loc, dy_loc, w_q, w_k, w_v, w_o)))
        return pl.pallas_call(
            finish,
            out_shape=(out, out),
            in_specs=[vmem] * 4,
            out_specs=(hbm, hbm),
            scratch_shapes=[pltpu.VMEM((rows, d_model), BF16),
                            pltpu.SemaphoreType.DMA((1 + PIECES,))],
            compiler_params=pltpu.CompilerParams(vmem_limit_bytes=8 * 1024 * 1024),
        )(y_v, acc, dk, wk)

    return jax.shard_map(local_body, mesh=mesh,
                         in_specs=(row_spec, row_spec, full_spec, full_spec, full_spec, full_spec),
                         out_specs=(row_spec, row_spec), check_vma=False)
```

```python
import functools
import math

import jax
import jax.numpy as jnp
from jax import lax
from jax.experimental import pallas as pl
from jax.experimental.pallas import tpu as pltpu
from jax.sharding import PartitionSpec as P

HEAD_DIM = 128
CHUNK = 128
SPLIT = 128
PIECES = 3
MESH = pl.DeviceIdType.MESH
F32 = jnp.float32
BF16 = jnp.bfloat16
NT = (((1,), (1,)), ((), ()))
NN = (((1,), (0,)), ((), ()))


def mm(a, b, dims=NN):
    return lax.dot_general(a, b, dims, preferred_element_type=F32)


def kernel(rows, d_model, q_heads, kv_heads,
           x_hbm, dy_hbm, wq_hbm, wk_hbm, wv_hbm, wo_hbm,
           y_v, dx_acc, dk_v, wk_v,
           x_v, dy_v, wq_v, wv_v, wo_v,
           qs, dot_v, k_all, v_all, kt, vt, pt, ds_t, e_buf, m_buf, l_buf, f_buf, o_v, dq_v,
           part, recv_a, recv_b, recv_c, send_c,
           in_sem, ag_send, ag_recv, rs_send, rs_recv):
    group = q_heads // kv_heads
    d = HEAD_DIM
    n_keys = 4 * rows
    half = group * rows
    scale = d ** -0.5
    gain = scale * math.log2(math.e)

    me = lax.axis_index("cp")
    core = lax.rem(me, 2)
    partner = me + 1 - 2 * core
    cross = lax.rem(me + 2, 4)

    barrier = pltpu.get_barrier_semaphore()
    for peer in (partner, cross):
        pl.semaphore_signal(barrier, inc=1, device_id={"cp": peer}, device_id_type=MESH)

    qcols = q_heads * d // 2
    loads = [
        pltpu.make_async_copy(wk_hbm, wk_v, in_sem.at[1]),
        pltpu.make_async_copy(x_hbm, x_v, in_sem.at[0]),
        pltpu.make_async_copy(wv_hbm, wv_v, in_sem.at[2]),
        pltpu.make_async_copy(wq_hbm.at[:, :qcols], wq_v.at[:, :qcols], in_sem.at[3]),
        pltpu.make_async_copy(wq_hbm.at[:, qcols:], wq_v.at[:, qcols:], in_sem.at[4]),
        pltpu.make_async_copy(dy_hbm, dy_v, in_sem.at[5]),
        pltpu.make_async_copy(wo_hbm.at[:qcols], wo_v.at[:qcols], in_sem.at[6]),
        pltpu.make_async_copy(wo_hbm.at[qcols:], wo_v.at[qcols:], in_sem.at[7]),
    ]
    for copy in loads:
        copy.start()

    def item(i):
        return (k_all if i % 2 == 0 else v_all).at[i // 2]

    def slot(i, s):
        return item(i).at[pl.ds(s * rows, rows)]

    def ag_copy(i, hop):
        src, dst, peer = ((0, 1, partner), (0, 2, cross), (2, 3, partner))[hop]
        return pltpu.make_async_remote_copy(
            src_ref=slot(i, src), dst_ref=slot(i, dst),
            send_sem=ag_send, recv_sem=ag_recv.at[i, hop],
            device_id={"cp": peer}, device_id_type=MESH)

    def forward(i):
        ag_copy(i, 1).wait_recv()
        ag_copy(i, 2).start()

    def transpose_item(i, ref):
        for s in range(4):
            ref[i // 2, :, s * rows:(s + 1) * rows] = slot(i, s)[...].T

    def head_of(i):
        h, j = i // group, i % group
        return h, slice(j * rows, (j + 1) * rows), slice(i * d, (i + 1) * d)

    def project_q(n):
        out = mm(x_v[...], wq_v[:, n * 2 * d:(n + 1) * 2 * d]).astype(BF16)
        for t in range(2):
            h, cols, _ = head_of(2 * n + t)
            qs[h, cols, :] = out[:, t * d:(t + 1) * d]

    def project_do(n):
        out = mm(wo_v[n * 2 * d:(n + 1) * 2 * d, :], dy_v[...], NT).astype(BF16)
        for t in range(2):
            h, cols, _ = head_of(2 * n + t)
            dot_v[h, :, cols] = out[t * d:(t + 1) * d, :]

    per_slot = rows // CHUNK

    def scores(i, s):
        h, cols, _ = head_of(i)
        j = i
        raw = mm(k_all[h, s * rows:(s + 1) * rows, :], qs[h, cols, :], NT)
        for c in range(per_slot):
            t = raw[c * CHUNK:(c + 1) * CHUNK].reshape(CHUNK // 8, 8, rows)
            m8 = jnp.max(t, axis=0) * gain
            e = jnp.exp2(t * gain - m8[None])
            e_buf[j, s * rows + c * CHUNK:s * rows + (c + 1) * CHUNK, :] = e.reshape(CHUNK, rows)
            m_buf[j, s * per_slot + c] = m8
            l_buf[j, s * per_slot + c] = jnp.sum(e, axis=0)

    def finalize(i, slots):
        h, cols, _ = head_of(i)
        j = i
        n_chunks = 4 * per_slot
        if 3 in slots:
            top = jnp.max(jnp.max(m_buf[j], axis=0), axis=0, keepdims=True)
            factor = [jnp.exp2(m_buf[j, c] - top) for c in range(n_chunks)]
            total = factor[0] * l_buf[j, 0]
            for c in range(1, n_chunks):
                total = total + factor[c] * l_buf[j, c]
            inv = 1.0 / jnp.sum(total, axis=0, keepdims=True)
            for c in range(n_chunks):
                f_buf[j, c] = factor[c] * inv
        for s in slots:
            for c in range(s * per_slot, (s + 1) * per_slot):
                e = e_buf[j, c * CHUNK:(c + 1) * CHUNK, :].reshape(CHUNK // 8, 8, rows)
                pt[h, c * CHUNK:(c + 1) * CHUNK, cols] = (e * f_buf[j, c][None]).reshape(CHUNK, rows).astype(BF16)

    def out_head(i):
        h, cols, feats = head_of(i)
        o_t = mm(vt[h], pt[h, :, cols]).astype(BF16)
        o_v[:, feats] = o_t.T
        return jnp.sum(dot_v[h, :, cols].astype(F32) * o_t.astype(F32), axis=0, keepdims=True)

    def dscore(i, delta):
        h, cols, _ = head_of(i)
        do_t = dot_v[h, :, cols]
        for s in range(4):
            keys = slice(s * rows, (s + 1) * rows)
            dp = mm(v_all[h, keys, :], do_t)
            ds_t[h, keys, cols] = (pt[h, keys, cols].astype(F32) * (dp - delta)).astype(BF16)

    def out_all(heads):
        heads = list(heads)
        delta = out_head(heads[0])
        for i, after in zip(heads, heads[1:] + [None]):
            delta_after = None if after is None else out_head(after)
            dscore(i, delta)
            delta = delta_after

    def dqs(i):
        h, cols, feats = head_of(i)
        dq_v[:, feats] = (mm(kt[h], ds_t[h, :, cols]) * scale).astype(BF16).T

    def grads(r, lo, hi):
        h = r % kv_heads
        for s in range(lo, hi):
            for t in range(rows // SPLIT):
                block = slice(s * rows + t * SPLIT, s * rows + (t + 1) * SPLIT)
                if r < kv_heads:
                    out = mm(pt[h, block, :], dot_v[h], NT)
                else:
                    out = mm(ds_t[h, block, :], qs[h])
                part[r, s, t * SPLIT:(t + 1) * SPLIT, :] = out

    def rs_copy(r, kind):
        src, dst, peer = ((part.at[r, 3], recv_a.at[r], partner),
                          (part.at[r, 1], recv_b.at[r], partner),
                          (send_c.at[r], recv_c.at[r], cross))[kind]
        return pltpu.make_async_remote_copy(
            src_ref=src, dst_ref=dst,
            send_sem=rs_send, recv_sem=rs_recv.at[r, kind],
            device_id={"cp": peer}, device_id_type=MESH)

    def reduce_cross(r):
        rs_copy(r, 0).wait_recv()
        send_c[r] = part[r, 2] + recv_a[r]
        rs_copy(r, 2).start()

    first = range(group)
    second = range(group, q_heads)
    n_pairs = q_heads // 4

    peers = [partner, cross]

    def stage(f):
        peers.reverse()
        pl.when(peers[0] != me)(f)

    def project_kv(w, kv_ref):
        out = mm(x_v[...], w[...]).astype(BF16)
        for h in range(kv_heads):
            kv_ref[h, :rows, :] = out[:, h * d:(h + 1) * d]

    def send_kv(item_of_head):
        for h in range(kv_heads):
            i = 2 * h + item_of_head
            ag_copy(i, 1).start()
            ag_copy(i, 0).start()

    @stage
    def _():
        loads[0].wait()
        loads[1].wait()
        project_kv(wk_v, k_all)

    pl.semaphore_wait(barrier, 2)
    send_kv(0)

    @stage
    def _():
        loads[2].wait()
        project_kv(wv_v, v_all)

    send_kv(1)

    @stage
    def _():
        loads[3].wait()
        for n in range(n_pairs):
            project_q(n)

    @stage
    def _():
        loads[4].wait()
        ag_copy(0, 0).wait_recv()
        for n in range(n_pairs):
            project_q(n_pairs + n)
            for i in (2 * n, 2 * n + 1):
                scores(i, 0)
                scores(i, 1)

    @stage
    def _():
        loads[5].wait()
        loads[6].wait()
        ag_copy(2, 0).wait_recv()
        for n in range(n_pairs):
            project_do(n)

    @stage
    def _():
        forward(0)
        for i in second:
            scores(i, 0)
            scores(i, 1)
        for n in first:
            scores(n, 2)

    def normalize_far(heads, r, filler=None):
        if filler is not None:
            for n in range(n_pairs):
                filler(n)
        for k, i in enumerate(heads):
            scores(i, 3)
            if k > 0:
                finalize(i - 1, (3, 2))
        finalize(heads[-1], (3, 2))
        grads(r, 3, 4)
        grads(r, 2, 3)
        rs_copy(r, 0).start()

    @stage
    def _():
        ag_copy(0, 2).wait_recv()
        normalize_far(first, 0)

    @stage
    def _():
        forward(2)
        for n in first:
            finalize(n, (1, 0))
            scores(group + n, 2)
        grads(0, 1, 2)

    @stage
    def _():
        reduce_cross(0)
        rs_copy(0, 1).start()
        forward(1)
        loads[7].wait()
        ag_copy(2, 2).wait_recv()
        normalize_far(second, 1, lambda n: project_do(n_pairs + n))

    @stage
    def _():
        forward(3)
        ag_copy(1, 0).wait_recv()
        ag_copy(1, 2).wait_recv()
        transpose_item(1, vt)
        for i in second:
            finalize(i, (1, 0))
        out_all(first[:group // 2])

    @stage
    def _():
        reduce_cross(1)
        out_all(first[group // 2:])
        grads(2, 3, 4)
        grads(2, 2, 3)
        rs_copy(2, 0).start()

    @stage
    def _():
        ag_copy(3, 0).wait_recv()
        ag_copy(3, 2).wait_recv()
        transpose_item(3, vt)
        grads(0, 0, 1)
        out_all(second[:group // 2])

    @stage
    def _():
        reduce_cross(2)
        out_all(second[group // 2:])
        grads(3, 3, 4)
        grads(3, 2, 3)
        rs_copy(3, 0).start()

    @stage
    def _():
        grads(1, 0, 2)
        grads(2, 0, 2)
        rs_copy(1, 1).start()
        rs_copy(2, 1).start()

    @stage
    def _():
        reduce_cross(3)
        grads(3, 0, 2)
        transpose_item(0, kt)
        for i in first:
            dqs(i)
        transpose_item(2, kt)
        for i in second:
            dqs(i)
        rs_copy(3, 1).start()
        for n in range(d_model // 256):
            cols = slice(n * 256, (n + 1) * 256)
            y_v[:, cols] = mm(o_v[...], wo_v[:, cols]).astype(BF16)

    def own(items, factor):
        parts = []
        for r in items:
            rs_copy(r, 1).wait_recv()
            rs_copy(r, 2).wait_recv()
        for r in items:
            total = part[r, 0] + recv_b[r] + recv_c[r]
            parts.append((total * factor).astype(BF16) if factor != 1 else total.astype(BF16))
        return jnp.concatenate(parts, axis=1)

    @stage
    def _():
        dv = own((0, 1), 1)
        for n in range(d_model // 256):
            cols = slice(n * 256, (n + 1) * 256)
            dx_acc[:, cols] = mm(dq_v[...], wq_v[cols, :], NT) + mm(dv, wv_v[cols, :], NT)

    pltpu.make_async_copy(x_v, x_v, ag_send).wait()

    @stage
    def _():
        dk_v[...] = own((2, 3), scale)

    pltpu.make_async_copy(dx_acc, dx_acc, rs_send).wait()


def finish(y_v, acc, dk, wk, y_hbm, dx_hbm, dx_v, sem):
    copies = [pltpu.make_async_copy(y_v, y_hbm, sem.at[0])]
    copies[0].start()
    width = acc.shape[1] // PIECES
    for n in range(PIECES):
        cols = slice(n * width, (n + 1) * width)
        dx_v[:, cols] = (acc[:, cols] + mm(dk[...], wk[cols, :], NT)).astype(BF16)
        copy = pltpu.make_async_copy(dx_v.at[:, cols], dx_hbm.at[:, cols], sem.at[1 + n])
        copy.start()
        copies.append(copy)
    for copy in copies:
        copy.wait()


def solution(mesh):
    row_spec = P(("dp", "cp"), None)
    full_spec = P(None, None)

    def local_body(x_loc, dy_loc, w_q, w_k, w_v, w_o):
        rows, d_model = x_loc.shape
        d = HEAD_DIM
        q_heads = w_q.shape[1] // d
        kv_heads = w_k.shape[1] // d
        group = q_heads // kv_heads
        n_keys = 4 * rows
        qw = q_heads * d
        hbm = pl.BlockSpec(memory_space=pltpu.HBM)
        vmem = pl.BlockSpec(memory_space=pltpu.VMEM)
        out = jax.ShapeDtypeStruct((rows, d_model), BF16)
        items = 2 * kv_heads
        y_v, acc, dk, wk = pl.pallas_call(
            functools.partial(kernel, rows, d_model, q_heads, kv_heads),
            out_shape=(out, jax.ShapeDtypeStruct((rows, d_model), F32),
                       jax.ShapeDtypeStruct((rows, kv_heads * d), BF16),
                       jax.ShapeDtypeStruct((d_model, kv_heads * d), BF16)),
            in_specs=[hbm] * 6,
            out_specs=(vmem,) * 4,
            scratch_shapes=[
                pltpu.VMEM((rows, d_model), BF16),
                pltpu.VMEM((rows, d_model), BF16),
                pltpu.VMEM((d_model, qw), BF16),
                pltpu.VMEM((d_model, kv_heads * d), BF16),
                pltpu.VMEM((qw, d_model), BF16),
                pltpu.VMEM((kv_heads, group * rows, d), BF16),
                pltpu.VMEM((kv_heads, d, group * rows), BF16),
                pltpu.VMEM((kv_heads, n_keys, d), BF16),
                pltpu.VMEM((kv_heads, n_keys, d), BF16),
                pltpu.VMEM((kv_heads, d, n_keys), BF16),
                pltpu.VMEM((kv_heads, d, n_keys), BF16),
                pltpu.VMEM((kv_heads, n_keys, group * rows), BF16),
                pltpu.VMEM((kv_heads, n_keys, group * rows), BF16),
                pltpu.VMEM((q_heads, n_keys, rows), F32),
                pltpu.VMEM((q_heads, n_keys // CHUNK, 8, rows), F32),
                pltpu.VMEM((q_heads, n_keys // CHUNK, 8, rows), F32),
                pltpu.VMEM((q_heads, n_keys // CHUNK, 8, rows), F32),
                pltpu.VMEM((rows, qw), BF16),
                pltpu.VMEM((rows, qw), BF16),
                pltpu.VMEM((items, 4, rows, d), F32),
                pltpu.VMEM((items, rows, d), F32),
                pltpu.VMEM((items, rows, d), F32),
                pltpu.VMEM((items, rows, d), F32),
                pltpu.VMEM((items, rows, d), F32),
                pltpu.SemaphoreType.DMA((8,)),
                pltpu.SemaphoreType.DMA,
                pltpu.SemaphoreType.DMA((items, 3)),
                pltpu.SemaphoreType.DMA,
                pltpu.SemaphoreType.DMA((items, 3)),
            ],
            compiler_params=pltpu.CompilerParams(
                collective_id=0, has_side_effects=True,
                vmem_limit_bytes=50 * 1024 * 1024),
        )(*(pltpu.with_memory_space_constraint(a, pltpu.HBM) for a in (x_loc, dy_loc, w_q, w_k, w_v, w_o)))
        return pl.pallas_call(
            finish,
            out_shape=(out, out),
            in_specs=[vmem] * 4,
            out_specs=(hbm, hbm),
            scratch_shapes=[pltpu.VMEM((rows, d_model), BF16),
                            pltpu.SemaphoreType.DMA((1 + PIECES,))],
            compiler_params=pltpu.CompilerParams(vmem_limit_bytes=8 * 1024 * 1024),
        )(y_v, acc, dk, wk)

    return jax.shard_map(local_body, mesh=mesh,
                         in_specs=(row_spec, row_spec, full_spec, full_spec, full_spec, full_spec),
                         out_specs=(row_spec, row_spec), check_vma=False)
```
